32 devices in a mesh: dp: 4 (over z), mx: 2 (over y), my: 4 (over x, core).
Axes of the slice: x: 2, y: 2, z: 4, core: 2. Of those that a mesh axis runs over, the one named last changes fastest.
Arguments:
- inputs: bfloat16 [768, 4096], P(('dp', 'mx', 'my')), may hold values from -6 to 6
- weight_means: bfloat16 [3, 14336, 4096], P(None, ('mx', 'my'), 'dp'), may hold values from -6 to 6
- weight_sigmas: bfloat16 [3, 14336, 4096], P(None, ('mx', 'my'), 'dp'), may hold values from 0.099609375 to 1
- weight_noise: bfloat16 [3, 14336, 4096], P(None, ('mx', 'my'), 'dp'), may hold values from -6 to 6
- input_signs: int32 [768, 4096], P(('dp', 'mx', 'my')), may hold values 0 or 1
- output_signs: int32 [2, 14336, 768], P(None, ('mx', 'my'), 'dp'), may hold values 0 or 1
- hidden_signs: int32 [14336, 768], P(('mx', 'my'), 'dp'), may hold values 0 or 1
- result_signs: int32 [768, 4096], P(('dp', 'mx', 'my')), may hold values 0 or 1
- cotangent: bfloat16 [768, 4096], P(('dp', 'mx', 'my')), may hold values from -6 to 6
Outputs:
- result: bfloat16 [768, 4096], P(('dp', 'mx', 'my'))
- input_grad: bfloat16 [768, 4096], P(('dp', 'mx', 'my'))
- mean_grad: bfloat16 [3, 14336, 4096], P(None, ('mx', 'my'), 'dp')
- sigma_grad: bfloat16 [3, 14336, 4096], P(None, ('mx', 'my'), 'dp')
The draws below stay inside these ranges and needn't reach their ends.
All inputs are finite; a program needn't handle non-finite values. No bound on the sum of `input_signs` or of `output_signs` or of `hidden_signs` or of `result_signs` on one device may be relied on, other than what follows from the above.
Results may differ from the reference program's by a relative error of at most 0.02.
Values may be sent and summed in bfloat16 or wider, within the bound.
A program may use at most 192 MiB of HBM per device.

```python
import math
import jax
import jax.numpy as jnp
from jax import lax

D = 4096
FF = 14336
TOK_DEV = 192
TOKENS = 768
N_DP = 4


def with_ends(array, own_key, least, largest):
    longest = array.shape.index(max(array.shape))
    spots = []
    for shift in (0, 1):
        where = [jax.random.randint(jax.random.fold_in(own_key, axis), (), 0, length) for axis, length in enumerate(array.shape)]
        where[longest] = (where[longest] + shift) % array.shape[longest]
        spots.append(tuple(where))
    return array.at[spots[0]].set(least).at[spots[1]].set(largest)


def levels(stream_key, dims, shards, low, top_value):
    def one(axis_at, shards_of):
        heights = jax.random.uniform(jax.random.fold_in(jax.random.fold_in(stream_key, 6), axis_at), (shards_of,), jnp.float32, low / len(shards), top_value / len(shards))
        return jnp.repeat(jnp.exp(heights), dims[axis_at] // shards_of).reshape((-1,) + (1,) * (len(dims) - axis_at - 1))

    level = one(*shards[0])
    for cut in shards[1:]:
        level = level * one(*cut)
    return level


def gaussian(own_key, shape, scale, bound, split=(), dtype=jnp.bfloat16):
    loudness = levels(own_key, shape, split, -0.22, 0.18) if split else 1.0
    drawn = jax.random.normal(own_key, shape, jnp.float32) * scale * loudness
    return jnp.minimum(jnp.maximum(drawn, -bound), bound).astype(dtype)


def setup_inputs(seed: int = 0) -> dict:
    key_of = jax.random.split(jax.random.key(seed), 10)
    inputs = gaussian(key_of[0], (TOKENS, D), 1.0, 6.0, ((0, 32),))
    weight_means = gaussian(key_of[1], (3, FF, D), 1.0, 6.0, ((1, 8), (2, 4)))
    weight_sigmas = jnp.clip(jnp.exp(math.log(1.0) - 2.306499 * jax.random.uniform(key_of[2], (3, FF, D), jnp.float32) ** levels(key_of[2], (3, FF, D), ((1, 8), (2, 4)), -0.2, 0.2)), 0.099609375, 1.0).astype(jnp.bfloat16)
    weight_noise = gaussian(key_of[3], (3, FF, D), 1.0, 6.0, ((1, 8), (2, 4)))
    input_signs = with_ends((jax.random.randint(key_of[4], (TOKENS, D), 0, 2) < 1).astype(jnp.int32), jax.random.fold_in(key_of[4], 1), 0, 1)
    output_signs = with_ends((jax.random.randint(key_of[5], (2, FF, TOKENS), 0, 2) < 1).astype(jnp.int32), jax.random.fold_in(key_of[5], 1), 0, 1)
    hidden_signs = with_ends((jax.random.randint(key_of[6], (FF, TOKENS), 0, 2) < 1).astype(jnp.int32), jax.random.fold_in(key_of[6], 1), 0, 1)
    result_signs = with_ends((jax.random.randint(key_of[7], (TOKENS, D), 0, 2) < 1).astype(jnp.int32), jax.random.fold_in(key_of[7], 1), 0, 1)
    cotangent = gaussian(key_of[8], (TOKENS, D), 1.0, 6.0, ((0, 32),))
    return {"inputs": inputs, "weight_means": weight_means, "weight_sigmas": weight_sigmas, "weight_noise": weight_noise, "input_signs": input_signs, "output_signs": output_signs, "hidden_signs": hidden_signs, "result_signs": result_signs, "cotangent": cotangent}


def to_sign(values):
    return (2 * values - 1).astype(jnp.float32)


def reference(inputs, weight_means, weight_sigmas, weight_noise, input_signs, output_signs, hidden_signs, result_signs, cotangent):
    scale_in = D ** -0.5
    scale_out = FF ** -0.5
    means_wide = jnp.swapaxes(weight_means, 1, 2)
    sigmas_wide = jnp.swapaxes(weight_sigmas, 1, 2)
    noise_wide = jnp.swapaxes(weight_noise, 1, 2)
    in_flip = to_sign(input_signs)
    out_flip = to_sign(jnp.transpose(output_signs, (2, 0, 1)))
    hid_flip = to_sign(hidden_signs.T)
    res_flip = to_sign(result_signs)
    perturb = (sigmas_wide.astype(jnp.float32) * noise_wide.astype(jnp.float32)).astype(jnp.bfloat16)
    flipped = (inputs.astype(jnp.float32) * in_flip).astype(jnp.bfloat16)
    gate = scale_in * jnp.dot(inputs, means_wide[0], preferred_element_type=jnp.float32) + scale_in * jnp.dot(flipped, perturb[0], preferred_element_type=jnp.float32) * out_flip[:, 0]
    up = scale_in * jnp.dot(inputs, means_wide[1], preferred_element_type=jnp.float32) + scale_in * jnp.dot(flipped, perturb[1], preferred_element_type=jnp.float32) * out_flip[:, 1]
    gate_sig = jax.nn.sigmoid(gate)
    hidden = (gate * gate_sig * up).astype(jnp.bfloat16)
    hid_flipped = (hidden.astype(jnp.float32) * hid_flip).astype(jnp.bfloat16)
    result = scale_out * jnp.dot(hidden, means_wide[2].T, preferred_element_type=jnp.float32) + scale_out * jnp.dot(hid_flipped, perturb[2].T, preferred_element_type=jnp.float32) * res_flip
    cot_flipped = (cotangent.astype(jnp.float32) * res_flip).astype(jnp.bfloat16)
    hid_grad = scale_out * jnp.dot(cotangent, means_wide[2], preferred_element_type=jnp.float32) + scale_out * jnp.dot(cot_flipped, perturb[2], preferred_element_type=jnp.float32) * hid_flip
    up_grad = (hid_grad * gate * gate_sig).astype(jnp.bfloat16)
    gate_grad = (hid_grad * up * gate_sig * (1.0 + gate * (1.0 - gate_sig))).astype(jnp.bfloat16)
    gate_flipped = (gate_grad.astype(jnp.float32) * out_flip[:, 0]).astype(jnp.bfloat16)
    up_flipped = (up_grad.astype(jnp.float32) * out_flip[:, 1]).astype(jnp.bfloat16)
    back_mean = jnp.dot(gate_grad, means_wide[0].T, preferred_element_type=jnp.float32) + jnp.dot(up_grad, means_wide[1].T, preferred_element_type=jnp.float32)
    back_pert = jnp.dot(gate_flipped, perturb[0].T, preferred_element_type=jnp.float32) + jnp.dot(up_flipped, perturb[1].T, preferred_element_type=jnp.float32)
    input_grad = scale_in * back_mean + scale_in * back_pert * in_flip
    mean_total = jnp.zeros((3, D, FF), jnp.float32)
    pert_total = jnp.zeros((3, D, FF), jnp.float32)
    for group in range(N_DP):
        lower = group * TOK_DEV
        upper = lower + TOK_DEV
        mean_terms = jnp.stack([
            scale_in * jnp.dot(inputs[lower:upper].T, gate_grad[lower:upper], preferred_element_type=jnp.float32),
            scale_in * jnp.dot(inputs[lower:upper].T, up_grad[lower:upper], preferred_element_type=jnp.float32),
            scale_out * jnp.dot(cotangent[lower:upper].T, hidden[lower:upper], preferred_element_type=jnp.float32)])
        pert_terms = jnp.stack([
            scale_in * jnp.dot(flipped[lower:upper].T, gate_flipped[lower:upper], preferred_element_type=jnp.float32),
            scale_in * jnp.dot(flipped[lower:upper].T, up_flipped[lower:upper], preferred_element_type=jnp.float32),
            scale_out * jnp.dot(cot_flipped[lower:upper].T, hid_flipped[lower:upper], preferred_element_type=jnp.float32)])
        mean_round = lax.optimization_barrier(mean_terms.astype(jnp.bfloat16))
        pert_round = lax.optimization_barrier(pert_terms.astype(jnp.bfloat16))
        mean_total = mean_total + mean_round.astype(jnp.float32)
        pert_total = pert_total + pert_round.astype(jnp.float32)
    mean_grad = jnp.swapaxes(mean_total.astype(jnp.bfloat16), 1, 2)
    sigma_grad = jnp.swapaxes((pert_total * noise_wide.astype(jnp.float32)).astype(jnp.bfloat16), 1, 2)
    return result.astype(jnp.bfloat16), input_grad.astype(jnp.bfloat16), mean_grad, sigma_grad
```

```python
import functools

import jax
import jax.numpy as jnp
from jax import lax
from jax.experimental import pallas as pl
from jax.experimental.pallas import tpu as pltpu
from jax.sharding import PartitionSpec as P

D = 4096
FF = 14336
MESH = pl.DeviceIdType.MESH
VMEM = pltpu.VMEM
DMA = pltpu.SemaphoreType.DMA


def to_sign(values):
    return (2 * values - 1).astype(jnp.bfloat16)


def dot(left, right, dims):
    return lax.dot_general(left, right, (dims, ((), ())), preferred_element_type=jnp.float32)


def remote(src, dst, send_sem, recv_sem, **where):
    return pltpu.make_async_remote_copy(
        src_ref=src, dst_ref=dst, send_sem=send_sem, recv_sem=recv_sem,
        device_id=where, device_id_type=MESH,
    )


def place():
    cores = 2 if lax.axis_size("my") % 2 == 0 else 1
    z, y, m = lax.axis_index("dp"), lax.axis_index("mx"), lax.axis_index("my")
    sizes = (lax.axis_size("dp"), lax.axis_size("mx"), lax.axis_size("my") // cores, cores)
    return (z, y, m // cores, m % cores), sizes


def greet_axes():
    (z, y, x, c), (nz, ny, nx, nc) = place()
    barrier = pltpu.get_barrier_semaphore()
    for d in range(1, nz):
        pl.semaphore_signal(barrier, inc=1, device_id={"dp": (z + d) % nz}, device_id_type=MESH)
    for d in range(1, ny):
        pl.semaphore_signal(barrier, inc=1, device_id={"mx": (y + d) % ny}, device_id_type=MESH)
    for d in range(1, nx):
        peer = ((x + d) % nx) * nc + c
        pl.semaphore_signal(barrier, inc=1, device_id={"my": peer}, device_id_type=MESH)
    for d in range(1, nc):
        peer = x * nc + (c + d) % nc
        pl.semaphore_signal(barrier, inc=1, device_id={"my": peer}, device_id_type=MESH)
    pl.semaphore_wait(barrier, nz + ny + nx + nc - 4)


class LineGather:
    def __init__(self, shard, full, s_sem, r_sem, own_sem):
        self.z, self.n = lax.axis_index("dp"), lax.axis_size("dp")
        self.shard, self.full, self.s_sem, self.r_sem = shard, full, s_sem, r_sem
        self.own = pltpu.make_async_copy(shard, full.at[self.z], own_sem)

    def copy(self, d, origin, src):
        return remote(
            src, self.full.at[origin], self.s_sem.at[d, origin], self.r_sem.at[d, origin],
            dp=(self.z + 1 - 2 * d + self.n) % self.n,
        )

    def begin(self):
        self.own.start()

        @pl.when(self.z < self.n - 1)
        def _():
            self.copy(0, self.z, self.shard).start()

        @pl.when(self.z > 0)
        def _():
            self.copy(1, self.z, self.shard).start()

    def relay(self, step):
        z, n = self.z, self.n
        for d in range(2):
            origin = z - step + 2 * d * step

            @pl.when((origin >= 0) & (origin < n))
            def _():
                copy = self.copy(d, origin, self.full.at[origin])
                copy.wait_recv()

                @pl.when((z < n - 1) if d == 0 else (z > 0))
                def _():
                    copy.start()

    def end(self):
        z, n = self.z, self.n
        self.own.wait()
        for origin in range(n):
            @pl.when((origin <= z) & (z < n - 1))
            def _():
                self.copy(0, origin, self.shard).wait_send()

            @pl.when((origin >= z) & (z > 0))
            def _():
                self.copy(1, origin, self.shard).wait_send()


def perturb_tiles(sigma, noise, out, wide, made, load, store):
    rows = made.shape[1]
    steps = out.shape[0] // rows

    def loads(i, slot):
        span = pl.ds(pl.multiple_of(i * rows, rows), rows)
        return (
            pltpu.make_async_copy(sigma.at[span], wide.at[slot, 0], load.at[slot, 0]),
            pltpu.make_async_copy(noise.at[span], wide.at[slot, 1], load.at[slot, 1]),
        )

    def stores(i, slot):
        span = pl.ds(pl.multiple_of(i * rows, rows), rows)
        return pltpu.make_async_copy(made.at[slot], out.at[span], store.at[slot])

    for copy in loads(0, 0):
        copy.start()

    def step(i, carry):
        slot = i % 2
        for copy in loads(i, slot):
            copy.wait()

        @pl.when(i + 1 < steps)
        def _():
            for copy in loads(i + 1, 1 - slot):
                copy.start()

        @pl.when(i >= 2)
        def _():
            stores(i - 2, slot).wait()

        product = wide[slot, 0].astype(jnp.float32) * wide[slot, 1].astype(jnp.float32)
        made[slot] = product.astype(made.dtype)
        stores(i, slot).start()
        return carry

    lax.fori_loop(0, steps, step, 0)
    for i in range(max(steps - 2, 0), steps):
        stores(i, i % 2).wait()


def spread_kernel(src, sigma, noise, shard, out, perturb, full, *scratch):
    z_s, z_r, a_s, a_r, b_s, b_r, c_s, c_r, own, g_s, g_r, g_own, wide, made, load, store = scratch
    (z, y, x, c), (nz, ny, nx, nc) = place()
    line = LineGather(shard, full, g_s, g_r, g_own)
    greet_axes()
    toward = 1 - 2 * ((2 * z) // nz)
    group = [(z + toward * k + nz) % nz for k in range(nz)]
    sends = []

    def start(copy):
        copy.start()
        sends.append(copy)
        return copy

    local = []
    for p in range(2):
        keep = pltpu.make_async_copy(src.at[p, :, z], out.at[p, :, z, y, x, c], own.at[p])
        keep.start()
        local.append(keep)
    for k in range(1, nz):
        for p in range(2):
            g = group[nz - k]
            start(remote(src.at[p, :, g], out.at[p, :, z, y, x, c], z_s.at[p, g], z_r.at[p, z], dp=g))

    def first(p, k):
        g = group[k]
        block = out.at[p, :, g, y, x, c]
        if k > 0:
            remote(src.at[p, :, g], block, z_s.at[p, g], z_r.at[p, g], dp=g).wait_recv()
        origin = src.at[p, :, g] if k == 0 else block
        if p == 0:
            return [
                start(remote(origin, block, a_s.at[p, g, e], a_r.at[p, g, e], my=((x + e) % nx) * nc + c))
                for e in range(1, nx)
            ]
        return [
            start(remote(origin, block, a_s.at[p, g, e], a_r.at[p, g, e], mx=(y + e) % ny))
            for e in range(1, ny)
        ]

    def second(p, k, before):
        g = group[k]
        for copy in before:
            copy.wait_recv()
        if k == 0:
            local[p].wait()
        if p == 0:
            block = out.at[p, :, g, y, :, c]
            return [
                start(remote(block, block, b_s.at[p, g, e], b_r.at[p, g, e], mx=(y + e) % ny))
                for e in range(1, ny)
            ]
        block = out.at[p, :, g, :, x, c]
        return [
            start(remote(block, block, b_s.at[p, g, e], b_r.at[p, g, e], my=((x + e) % nx) * nc + c))
            for e in range(1, nx)
        ]

    def third(p, k, before):
        g = group[k]
        for copy in before:
            copy.wait_recv()
        block = out.at[p, :, g, :, :, c]
        return [
            start(remote(block, block, c_s.at[p, g, e], c_r.at[p, g, e], my=x * nc + (c + e) % nc))
            for e in range(1, nc)
        ]

    a, b, last = {}, {}, []
    for p in range(2):
        a[p, 0] = first(p, 0)
    line.begin()
    perturb_tiles(sigma, noise, perturb, wide, made, load, store)
    for k in range(nz + 2):
        for p in range(2):
            if 0 < k < nz:
                a[p, k] = first(p, k)
            if 0 <= k - 1 < nz:
                b[p, k - 1] = second(p, k - 1, a[p, k - 1])
            if 0 <= k - 2 < nz:
                last += third(p, k - 2, b[p, k - 2])
        if k >= 3:
            line.relay(k - 2)
    for copy in last:
        copy.wait_recv()
    for copy in sends:
        copy.wait_send()
    line.end()


def spread(pairs, sigma, noise, shard):
    nz, ny, nx = lax.axis_size("dp"), lax.axis_size("mx"), lax.axis_size("my")
    nc = 2 if nx % 2 == 0 else 1
    nx //= nc
    _, _, _, rows, width = pairs.shape
    most = max(nx, ny)
    planes, hid, _ = sigma.shape
    tile = 256 if hid % 256 == 0 else hid
    flat = (planes * hid, width)
    anywhere = pl.BlockSpec(memory_space=pl.ANY)
    within = pl.BlockSpec(memory_space=VMEM)
    bf16 = jnp.bfloat16
    return pl.pallas_call(
        spread_kernel,
        out_shape=[
            jax.ShapeDtypeStruct((2, 2, nz, ny, nx, nc, rows, width), bf16),
            jax.ShapeDtypeStruct(flat, bf16),
            jax.ShapeDtypeStruct((nz,) + shard.shape, bf16),
        ],
        in_specs=[anywhere, anywhere, anywhere, within],
        out_specs=[anywhere, anywhere, within],
        scratch_shapes=[
            DMA((2, nz)), DMA((2, nz)),
            DMA((2, nz, most)), DMA((2, nz, most)),
            DMA((2, nz, most)), DMA((2, nz, most)),
            DMA((2, nz, nc)), DMA((2, nz, nc)),
            DMA((2,)),
            DMA((2, nz)), DMA((2, nz)), DMA,
            VMEM((2, 2, tile, width), bf16),
            VMEM((2, tile, width), bf16),
            DMA((2, 2)), DMA((2,)),
        ],
        compiler_params=pltpu.CompilerParams(
            collective_id=1, has_side_effects=True, vmem_limit_bytes=60 * 2**20
        ),
        cost_estimate=pl.CostEstimate(flops=10**10, bytes_accessed=10**7, transcendentals=0),
        name="spread",
    )(pairs, sigma.reshape(flat), noise.reshape(flat), shard)


def project_kernel(scale, k, half, gathered, means, perturb, signs, shard, out, full, *scratch):
    x, a, m, p, s, part, send, recv, s_sem, r_sem, load, g_s, g_r, g_own = scratch
    line = LineGather(shard, full, g_s, g_r, g_own)
    z, n = lax.axis_index("dp"), lax.axis_size("dp")
    rows, hid = out.shape
    sources = (gathered.at[half, 0], gathered.at[half, 1], means.at[k], perturb.at[k], signs)
    loads = [
        pltpu.make_async_copy(source, target, load.at[i])
        for i, (source, target) in enumerate(zip(sources, (x, a, m, p, s)))
    ]
    for copy in loads:
        copy.start()
    tile = 256 if hid % 256 == 0 else hid
    barrier = pltpu.get_barrier_semaphore()

    @pl.when(z > 0)
    def _():
        pl.semaphore_signal(barrier, inc=1, device_id={"dp": z - 1}, device_id_type=MESH)

    @pl.when(z < n - 1)
    def _():
        pl.semaphore_signal(barrier, inc=1, device_id={"dp": z + 1}, device_id_type=MESH)

    inner = (z > 0) & (z < n - 1)

    @pl.when(inner)
    def _():
        pl.semaphore_wait(barrier, 2)

    @pl.when(jnp.logical_not(inner) & (n > 1))
    def _():
        pl.semaphore_wait(barrier, 1)

    line.begin()
    for copy in loads:
        copy.wait()

    def tiles(body):
        def step(j, carry):
            body(pl.ds(pl.multiple_of(j * tile, tile), tile))
            return carry

        lax.fori_loop(0, hid // tile, step, 0)

    def compute(g):
        span = pl.ds(pl.multiple_of(g * rows, rows), rows)

        def body(cols):
            left = x[span, :]
            mean = dot(left, m[cols, :], ((1,), (1,)))
            pert = dot(left * a[span, :], p[cols, :], ((1,), (1,)))
            part[:, cols] = scale * mean + scale * pert * s[g, :, cols].astype(jnp.float32)

        tiles(body)

    def copy(d, g):
        return remote(
            send.at[g], recv.at[d, g], s_sem.at[g], r_sem.at[d, g], dp=(z + 1 - 2 * d + n) % n
        )

    def slot(i, carry):
        t, d = i // 2, i % 2
        behind = z + d * (n - 1 - 2 * z)
        ahead = n - 1 - behind

        @pl.when((t >= behind) & (ahead > 0))
        def _():
            g = (1 - d) * (n - 1 - t + z) + d * (t - (n - 1 - z))
            compute(g)

            @pl.when(behind > 0)
            def _():
                copy(d, g).wait_recv()

                def body(cols):
                    total = part[:, cols] + recv[d, g, :, cols].astype(jnp.float32)
                    send[g, :, cols] = total.astype(send.dtype)

                tiles(body)

            @pl.when(behind == 0)
            def _():
                def body(cols):
                    send[g, :, cols] = part[:, cols].astype(send.dtype)

                tiles(body)

            copy(d, g).start()

        @pl.when(d == 1)
        def _():
            line.relay(t + 1)

        return carry

    lax.fori_loop(0, 2 * (n - 1), slot, 0)
    compute(z)

    @pl.when(z > 0)
    def _():
        copy(0, z).wait_recv()

        def body(cols):
            part[:, cols] = part[:, cols] + recv[0, z, :, cols].astype(jnp.float32)

        tiles(body)

    @pl.when(z < n - 1)
    def _():
        copy(1, z).wait_recv()

        def body(cols):
            part[:, cols] = part[:, cols] + recv[1, z, :, cols].astype(jnp.float32)

        tiles(body)

    def body(cols):
        out[:, cols] = part[:, cols]

    tiles(body)
    for g in range(n):
        @pl.when(z != g)
        def _():
            copy(0, g).wait_send()

    line.end()


def project(cid, k, half, scale, gathered, means, perturb, signs, shard):
    n = lax.axis_size("dp")
    tokens, width = gathered.shape[2:]
    hid = means.shape[1]
    rows = tokens // n
    return pl.pallas_call(
        functools.partial(project_kernel, scale, k, half),
        out_shape=[
            jax.ShapeDtypeStruct((rows, hid), jnp.float32),
            jax.ShapeDtypeStruct((n, rows, hid), jnp.bfloat16),
        ],
        in_specs=[pl.BlockSpec(memory_space=pl.ANY)] * 4 + [pl.BlockSpec(memory_space=VMEM)],
        out_specs=[pl.BlockSpec(memory_space=VMEM)] * 2,
        scratch_shapes=[
            VMEM((tokens, width), jnp.bfloat16),
            VMEM((tokens, width), jnp.bfloat16),
            VMEM((hid, width), jnp.bfloat16),
            VMEM((hid, width), jnp.bfloat16),
            VMEM((n, rows, hid), jnp.bfloat16),
            VMEM((rows, hid), jnp.float32),
            VMEM((n, rows, hid), jnp.bfloat16),
            VMEM((2, n, rows, hid), jnp.bfloat16),
            DMA((n,)),
            DMA((2, n)),
            DMA((5,)),
            DMA((2, n)),
            DMA((2, n)),
            DMA,
        ],
        compiler_params=pltpu.CompilerParams(
            collective_id=cid, has_side_effects=True, vmem_limit_bytes=60 * 2**20
        ),
        cost_estimate=pl.CostEstimate(flops=2 * 10**10, bytes_accessed=10**7, transcendentals=0),
        name=f"project{k}",
    )(gathered, means, perturb, signs, shard)


def finish_kernel(t, out, a1, rc, rx, ry, b0, b1, r0, r1, fin, s_sem, r_sem):
    (z, y, x, c), (nz, ny, nx, nc) = place()
    width = t.shape[-1]
    half = width // 2
    f32, bf16 = jnp.float32, jnp.bfloat16
    lo, hi = pl.ds(0, half), pl.ds(half, half)
    greet_axes()
    sends = []
    count = [0]

    def start(src, dst, **where):
        i = count[0]
        count[0] += 1
        copy = remote(src, dst, s_sem.at[i], r_sem.at[i], **where)
        copy.start()
        sends.append(copy)
        return copy

    def groups(body):
        def step(g, carry):
            body(g)
            return carry

        lax.fori_loop(0, nz, step, 0)

    wait = [
        start(t.at[:, :, :, (c + e) % nc], rc.at[e - 1], my=x * nc + (c + e) % nc) for e in range(1, nc)
    ]
    for copy in wait:
        copy.wait_recv()

    def add_cores(g):
        for i in range(ny):
            for j in range(nx):
                total = t[g, i, j, c].astype(f32)
                for e in range(nc - 1):
                    total = total + rc[e, g, i, j].astype(f32)
                a1[g, i, j] = total.astype(bf16)

    groups(add_cores)
    wait = [
        start(a1.at[:, :, (x + e) % nx, :, lo], rx.at[e - 1], my=((x + e) % nx) * nc + c)
        for e in range(1, nx)
    ]
    wait += [
        start(a1.at[:, (y + e) % ny, :, :, hi], ry.at[e - 1], mx=(y + e) % ny) for e in range(1, ny)
    ]
    for copy in wait:
        copy.wait_recv()

    def mine(g, i, j, cols):
        total = t[g, i, j, c, :, cols].astype(f32)
        for e in range(nc - 1):
            total = total + rc[e, g, i, j, :, cols].astype(f32)
        return total

    def low(g, i):
        total = mine(g, i, x, lo)
        for e in range(nx - 1):
            total = total + rx[e, g, i].astype(f32)
        return total

    def high(g, j):
        total = mine(g, y, j, hi)
        for e in range(ny - 1):
            total = total + ry[e, g, j].astype(f32)
        return total

    def add_first(g):
        for i in range(ny):
            b0[i, g] = low(g, i).astype(bf16)
        for j in range(nx):
            b1[j, g] = high(g, j).astype(bf16)

    groups(add_first)
    wait = [start(b0.at[(y + e) % ny], r0.at[e - 1], mx=(y + e) % ny) for e in range(1, ny)]
    wait += [
        start(b1.at[(x + e) % nx], r1.at[e - 1], my=((x + e) % nx) * nc + c) for e in range(1, nx)
    ]
    for copy in wait:
        copy.wait_recv()

    def add_second(g):
        total = low(g, y)
        for e in range(ny - 1):
            total = total + r0[e, g].astype(f32)
        fin[g, :, lo] = total.astype(bf16)
        total = high(g, x)
        for e in range(nx - 1):
            total = total + r1[e, g].astype(f32)
        fin[g, :, hi] = total.astype(bf16)

    groups(add_second)
    cols = pl.ds(pl.multiple_of(z * width, width), width)
    wait = [start(fin.at[(z + d) % nz], out.at[:, cols], dp=(z + d) % nz) for d in range(1, nz)]
    out[:, cols] = fin[z]
    for copy in wait:
        copy.wait_recv()
    for copy in sends:
        copy.wait_send()


def finish(cid, total):
    nz, ny, nx = lax.axis_size("dp"), lax.axis_size("mx"), lax.axis_size("my")
    nc = 2 if nx % 2 == 0 else 1
    nx //= nc
    tokens, width = total.shape
    rows = tokens // (nz * ny * nx * nc)
    half = width // 2
    copies = nz + ny * 2 + nx * 2 + nc
    bf16 = jnp.bfloat16
    return pl.pallas_call(
        finish_kernel,
        out_shape=jax.ShapeDtypeStruct((rows, nz * width), bf16),
        in_specs=[pl.BlockSpec(memory_space=VMEM)],
        out_specs=pl.BlockSpec(memory_space=VMEM),
        scratch_shapes=[
            VMEM((nz, ny, nx, rows, width), bf16),
            VMEM((max(nc - 1, 1), nz, ny, nx, rows, width), bf16),
            VMEM((max(nx - 1, 1), nz, ny, rows, half), bf16),
            VMEM((max(ny - 1, 1), nz, nx, rows, half), bf16),
            VMEM((ny, nz, rows, half), bf16),
            VMEM((nx, nz, rows, half), bf16),
            VMEM((max(ny - 1, 1), nz, rows, half), bf16),
            VMEM((max(nx - 1, 1), nz, rows, half), bf16),
            VMEM((nz, rows, width), bf16),
            DMA((copies,)),
            DMA((copies,)),
        ],
        compiler_params=pltpu.CompilerParams(
            collective_id=cid, has_side_effects=True, vmem_limit_bytes=32 * 2**20
        ),
        cost_estimate=pl.CostEstimate(flops=10**10, bytes_accessed=10**7, transcendentals=0),
        name=f"finish{cid}",
    )(total.reshape(nz, ny, nx, nc, rows, width))


def grad_kernel(groups, scale, hid, sign, x, a, noise, *rest):
    mean, sigma = rest[-2:]
    rows = x.shape[0] // groups
    total_mean = total_pert = None
    for g in range(groups):
        part = slice(g * rows, (g + 1) * rows)
        left = hid[part, :]
        right = x[part, :]
        m = (scale * dot(left, right, ((0,), (0,)))).astype(jnp.bfloat16)
        p = (scale * dot(left * sign[part, :], right * a[part, :], ((0,), (0,)))).astype(jnp.bfloat16)
        m, p = m.astype(jnp.float32), p.astype(jnp.float32)
        total_mean = m if g == 0 else total_mean + m
        total_pert = p if g == 0 else total_pert + p
    mean[...] = total_mean.astype(jnp.bfloat16)
    sigma[...] = (total_pert * noise[...].astype(jnp.float32)).astype(jnp.bfloat16)


def weight_grads(groups, k, half, scale, hid, sign, gathered, noise, into):
    tokens, ff = hid.shape
    width = gathered.shape[3]
    tile = 256 if ff % 256 == 0 else ff
    whole = lambda j: pl.BlockSpec((None, None, tokens, width), lambda i: (half, j, 0, 0))
    block = pl.BlockSpec((None, tile, width), lambda i: (k, i, 0))
    cols = pl.BlockSpec((tokens, tile), lambda i: (0, i))
    keep = [pl.BlockSpec(memory_space=pl.ANY)] * len(into)
    return pl.pallas_call(
        functools.partial(grad_kernel, groups, scale),
        grid=(ff // tile,),
        out_shape=[jax.ShapeDtypeStruct(noise.shape, jnp.bfloat16)] * 2,
        in_specs=[cols, cols, whole(0), whole(1), block] + keep,
        out_specs=[block, block],
        input_output_aliases={5 + i: i for i in range(len(into))},
        cost_estimate=pl.CostEstimate(
            flops=4 * tokens * ff * width, bytes_accessed=6 * ff * width, transcendentals=0
        ),
        name=f"grads{k}",
    )(hid, sign, gathered, gathered, noise, *into)


def on_device(
    inputs,
    weight_means,
    weight_sigmas,
    weight_noise,
    input_signs,
    output_signs,
    hidden_signs,
    result_signs,
    cotangent,
):
    f32, bf16 = jnp.float32, jnp.bfloat16
    scale_in = D ** (-0.5)
    scale_out = FF ** (-0.5)
    groups = lax.axis_size("dp")

    def share(value):
        return lax.all_gather(value, "dp", axis=0, tiled=True)

    rows, full = inputs.shape
    width = full // groups
    pairs = jnp.stack([inputs, to_sign(input_signs), cotangent, to_sign(result_signs)])
    pairs = pairs.reshape(2, 2, rows, groups, width).swapaxes(2, 3)
    own_s0, own_s1 = to_sign(output_signs[0]).T, to_sign(output_signs[1]).T
    own_s2 = to_sign(hidden_signs).T
    gathered, perturb, s0 = spread(pairs, weight_sigmas, weight_noise, own_s0)
    gathered = gathered.reshape(2, 2, -1, width)
    perturb = perturb.reshape(weight_sigmas.shape)
    a, r = gathered[0, 1], gathered[1, 1]

    gate, s1 = project(2, 0, 0, scale_in, gathered, weight_means, perturb, s0, own_s1)
    up, s2 = project(3, 1, 0, scale_in, gathered, weight_means, perturb, s1, own_s2)
    gate_sig = jax.nn.sigmoid(gate)
    hidden = (gate * gate_sig * up).astype(bf16)
    hid_grad, hidden = project(4, 2, 1, scale_out, gathered, weight_means, perturb, s2, hidden)
    up_grad = share((hid_grad * gate * gate_sig).astype(bf16))
    gate_grad = share(
        (hid_grad * up * gate_sig * (1.0 + gate * (1.0 - gate_sig))).astype(bf16)
    )
    hidden, s0, s1, s2 = (v.reshape(-1, v.shape[2]) for v in (hidden, s0, s1, s2))

    def back(k, value, sign):
        return (
            dot(value, weight_means[k], ((1,), (0,))),
            dot(value * sign, perturb[k], ((1,), (0,))),
        )

    mean, pert = back(2, hidden, s2)
    result = finish(5, (scale_out * mean + scale_out * pert * r.astype(f32)).astype(bf16))
    grads = weight_grads(groups, 2, 1, scale_out, hidden, s2, gathered, weight_noise, ())
    up_grad, result, *grads = lax.optimization_barrier((up_grad, result, *grads))
    up_mean, up_pert = back(1, up_grad, s1)
    grads = weight_grads(groups, 1, 0, scale_in, up_grad, s1, gathered, weight_noise, grads)
    gate_grad, up_mean, up_pert, *grads = lax.optimization_barrier(
        (gate_grad, up_mean, up_pert, *grads)
    )
    gate_mean, gate_pert = back(0, gate_grad, s0)
    input_grad = finish(
        6,
        (
            scale_in * (gate_mean + up_mean) + scale_in * (gate_pert + up_pert) * a.astype(f32)
        ).astype(bf16),
    )
    mean_grad, sigma_grad = weight_grads(
        groups, 0, 0, scale_in, gate_grad, s0, gathered, weight_noise, grads
    )
    return (result, input_grad, mean_grad, sigma_grad)


def solution(mesh):
    return jax.shard_map(
        on_device,
        mesh=mesh,
        in_specs=(
            P(("dp", "mx", "my"), None),
            P(None, ("mx", "my"), "dp"),
            P(None, ("mx", "my"), "dp"),
            P(None, ("mx", "my"), "dp"),
            P(("dp", "mx", "my"), None),
            P(None, ("mx", "my"), "dp"),
            P(("mx", "my"), "dp"),
            P(("dp", "mx", "my"), None),
            P(("dp", "mx", "my"), None),
        ),
        out_specs=(
            P(("dp", "mx", "my"), None),
            P(("dp", "mx", "my"), None),
            P(None, ("mx", "my"), "dp"),
            P(None, ("mx", "my"), "dp"),
        ),
        check_vma=False,
    )
```

```python
import functools

import jax
import jax.numpy as jnp
from jax import lax
from jax.experimental import pallas as pl
from jax.experimental.pallas import tpu as pltpu
from jax.sharding import PartitionSpec as P

D = 4096
FF = 14336
MESH = pl.DeviceIdType.MESH
VMEM = pltpu.VMEM
DMA = pltpu.SemaphoreType.DMA


def to_sign(values):
    return (2 * values - 1).astype(jnp.bfloat16)


def dot(left, right, dims):
    return lax.dot_general(left, right, (dims, ((), ())), preferred_element_type=jnp.float32)


def remote(src, dst, send_sem, recv_sem, **where):
    return pltpu.make_async_remote_copy(
        src_ref=src, dst_ref=dst, send_sem=send_sem, recv_sem=recv_sem,
        device_id=where, device_id_type=MESH,
    )


def place():
    cores = 2 if lax.axis_size("my") % 2 == 0 else 1
    z, y, m = lax.axis_index("dp"), lax.axis_index("mx"), lax.axis_index("my")
    sizes = (lax.axis_size("dp"), lax.axis_size("mx"), lax.axis_size("my") // cores, cores)
    return (z, y, m // cores, m % cores), sizes


def greet_axes():
    (z, y, x, c), (nz, ny, nx, nc) = place()
    barrier = pltpu.get_barrier_semaphore()
    for d in range(1, nz):
        pl.semaphore_signal(barrier, inc=1, device_id={"dp": (z + d) % nz}, device_id_type=MESH)
    for d in range(1, ny):
        pl.semaphore_signal(barrier, inc=1, device_id={"mx": (y + d) % ny}, device_id_type=MESH)
    for d in range(1, nx):
        peer = ((x + d) % nx) * nc + c
        pl.semaphore_signal(barrier, inc=1, device_id={"my": peer}, device_id_type=MESH)
    for d in range(1, nc):
        peer = x * nc + (c + d) % nc
        pl.semaphore_signal(barrier, inc=1, device_id={"my": peer}, device_id_type=MESH)
    pl.semaphore_wait(barrier, nz + ny + nx + nc - 4)


class LineGather:
    def __init__(self, shard, full, s_sem, r_sem, own_sem):
        self.z, self.n = lax.axis_index("dp"), lax.axis_size("dp")
        self.shard, self.full, self.s_sem, self.r_sem = shard, full, s_sem, r_sem
        self.own = pltpu.make_async_copy(shard, full.at[self.z], own_sem)

    def copy(self, d, origin, src):
        return remote(
            src, self.full.at[origin], self.s_sem.at[d, origin], self.r_sem.at[d, origin],
            dp=(self.z + 1 - 2 * d + self.n) % self.n,
        )

    def begin(self):
        self.own.start()

        @pl.when(self.z < self.n - 1)
        def _():
            self.copy(0, self.z, self.shard).start()

        @pl.when(self.z > 0)
        def _():
            self.copy(1, self.z, self.shard).start()

    def relay(self, step):
        z, n = self.z, self.n
        for d in range(2):
            origin = z - step + 2 * d * step

            @pl.when((origin >= 0) & (origin < n))
            def _():
                copy = self.copy(d, origin, self.full.at[origin])
                copy.wait_recv()

                @pl.when((z < n - 1) if d == 0 else (z > 0))
                def _():
                    copy.start()

    def end(self):
        z, n = self.z, self.n
        self.own.wait()
        for origin in range(n):
            @pl.when((origin <= z) & (z < n - 1))
            def _():
                self.copy(0, origin, self.shard).wait_send()

            @pl.when((origin >= z) & (z > 0))
            def _():
                self.copy(1, origin, self.shard).wait_send()


def perturb_tiles(sigma, noise, out, wide, made, load, store):
    rows = made.shape[1]
    steps = out.shape[0] // rows

    def loads(i, slot):
        span = pl.ds(pl.multiple_of(i * rows, rows), rows)
        return (
            pltpu.make_async_copy(sigma.at[span], wide.at[slot, 0], load.at[slot, 0]),
            pltpu.make_async_copy(noise.at[span], wide.at[slot, 1], load.at[slot, 1]),
        )

    def stores(i, slot):
        span = pl.ds(pl.multiple_of(i * rows, rows), rows)
        return pltpu.make_async_copy(made.at[slot], out.at[span], store.at[slot])

    for copy in loads(0, 0):
        copy.start()

    def step(i, carry):
        slot = i % 2
        for copy in loads(i, slot):
            copy.wait()

        @pl.when(i + 1 < steps)
        def _():
            for copy in loads(i + 1, 1 - slot):
                copy.start()

        @pl.when(i >= 2)
        def _():
            stores(i - 2, slot).wait()

        product = wide[slot, 0].astype(jnp.float32) * wide[slot, 1].astype(jnp.float32)
        made[slot] = product.astype(made.dtype)
        stores(i, slot).start()
        return carry

    lax.fori_loop(0, steps, step, 0)
    for i in range(max(steps - 2, 0), steps):
        stores(i, i % 2).wait()


def spread_kernel(src, sigma, noise, shard, out, perturb, full, *scratch):
    z_s, z_r, a_s, a_r, b_s, b_r, c_s, c_r, own, g_s, g_r, g_own, wide, made, load, store = scratch
    (z, y, x, c), (nz, ny, nx, nc) = place()
    line = LineGather(shard, full, g_s, g_r, g_own)
    greet_axes()
    toward = 1 - 2 * ((2 * z) // nz)
    group = [(z + toward * k + nz) % nz for k in range(nz)]
    sends = []

    def start(copy):
        copy.start()
        sends.append(copy)
        return copy

    local = []
    for p in range(2):
        keep = pltpu.make_async_copy(src.at[p, :, z], out.at[p, :, z, y, x, c], own.at[p])
        keep.start()
        local.append(keep)
    for k in range(1, nz):
        for p in range(2):
            g = group[nz - k]
            start(remote(src.at[p, :, g], out.at[p, :, z, y, x, c], z_s.at[p, g], z_r.at[p, z], dp=g))

    def first(p, k):
        g = group[k]
        block = out.at[p, :, g, y, x, c]
        if k > 0:
            remote(src.at[p, :, g], block, z_s.at[p, g], z_r.at[p, g], dp=g).wait_recv()
        origin = src.at[p, :, g] if k == 0 else block
        if p == 0:
            return [
                start(remote(origin, block, a_s.at[p, g, e], a_r.at[p, g, e], my=((x + e) % nx) * nc + c))
                for e in range(1, nx)
            ]
        return [
            start(remote(origin, block, a_s.at[p, g, e], a_r.at[p, g, e], mx=(y + e) % ny))
            for e in range(1, ny)
        ]

    def second(p, k, before):
        g = group[k]
        for copy in before:
            copy.wait_recv()
        if k == 0:
            local[p].wait()
        if p == 0:
            block = out.at[p, :, g, y, :, c]
            return [
                start(remote(block, block, b_s.at[p, g, e], b_r.at[p, g, e], mx=(y + e) % ny))
                for e in range(1, ny)
            ]
        block = out.at[p, :, g, :, x, c]
        return [
            start(remote(block, block, b_s.at[p, g, e], b_r.at[p, g, e], my=((x + e) % nx) * nc + c))
            for e in range(1, nx)
        ]

    def third(p, k, before):
        g = group[k]
        for copy in before:
            copy.wait_recv()
        block = out.at[p, :, g, :, :, c]
        return [
            start(remote(block, block, c_s.at[p, g, e], c_r.at[p, g, e], my=x * nc + (c + e) % nc))
            for e in range(1, nc)
        ]

    a, b, last = {}, {}, []
    for p in range(2):
        a[p, 0] = first(p, 0)
    line.begin()
    perturb_tiles(sigma, noise, perturb, wide, made, load, store)
    for k in range(1, nz):
        for p in range(2):
            a[p, k] = first(p, k)
    for p in range(2):
        b[p, 0] = second(p, 0, a[p, 0])
    line.relay(1)
    for k in range(1, nz):
        for p in range(2):
            b[p, k] = second(p, k, a[p, k])
    for p in range(2):
        last += third(p, 0, b[p, 0])
    line.relay(2)
    for k in range(1, nz):
        for p in range(2):
            last += third(p, k, b[p, k])
    for step in range(3, nz):
        line.relay(step)
    for copy in last:
        copy.wait_recv()
    for copy in sends:
        copy.wait_send()
    line.end()


def spread(pairs, sigma, noise, shard):
    nz, ny, nx = lax.axis_size("dp"), lax.axis_size("mx"), lax.axis_size("my")
    nc = 2 if nx % 2 == 0 else 1
    nx //= nc
    _, _, _, rows, width = pairs.shape
    most = max(nx, ny)
    planes, hid, _ = sigma.shape
    tile = 256 if hid % 256 == 0 else hid
    flat = (planes * hid, width)
    anywhere = pl.BlockSpec(memory_space=pl.ANY)
    within = pl.BlockSpec(memory_space=VMEM)
    bf16 = jnp.bfloat16
    return pl.pallas_call(
        spread_kernel,
        out_shape=[
            jax.ShapeDtypeStruct((2, 2, nz, ny, nx, nc, rows, width), bf16),
            jax.ShapeDtypeStruct(flat, bf16),
            jax.ShapeDtypeStruct((nz,) + shard.shape, bf16),
        ],
        in_specs=[anywhere, anywhere, anywhere, within],
        out_specs=[anywhere, anywhere, within],
        scratch_shapes=[
            DMA((2, nz)), DMA((2, nz)),
            DMA((2, nz, most)), DMA((2, nz, most)),
            DMA((2, nz, most)), DMA((2, nz, most)),
            DMA((2, nz, nc)), DMA((2, nz, nc)),
            DMA((2,)),
            DMA((2, nz)), DMA((2, nz)), DMA,
            VMEM((2, 2, tile, width), bf16),
            VMEM((2, tile, width), bf16),
            DMA((2, 2)), DMA((2,)),
        ],
        compiler_params=pltpu.CompilerParams(
            collective_id=1, has_side_effects=True, vmem_limit_bytes=60 * 2**20
        ),
        cost_estimate=pl.CostEstimate(flops=10**10, bytes_accessed=10**7, transcendentals=0),
        name="spread",
    )(pairs, sigma.reshape(flat), noise.reshape(flat), shard)


def project_kernel(scale, k, half, gathered, means, perturb, signs, shard, out, full, *scratch):
    x, a, m, p, s, part, send, recv, s_sem, r_sem, load, g_s, g_r, g_own = scratch
    line = LineGather(shard, full, g_s, g_r, g_own)
    z, n = lax.axis_index("dp"), lax.axis_size("dp")
    rows, hid = out.shape
    sources = (gathered.at[half, 0], gathered.at[half, 1], means.at[k], perturb.at[k], signs)
    loads = [
        pltpu.make_async_copy(source, target, load.at[i])
        for i, (source, target) in enumerate(zip(sources, (x, a, m, p, s)))
    ]
    for copy in loads:
        copy.start()
    tile = 256 if hid % 256 == 0 else hid
    barrier = pltpu.get_barrier_semaphore()

    @pl.when(z > 0)
    def _():
        pl.semaphore_signal(barrier, inc=1, device_id={"dp": z - 1}, device_id_type=MESH)

    @pl.when(z < n - 1)
    def _():
        pl.semaphore_signal(barrier, inc=1, device_id={"dp": z + 1}, device_id_type=MESH)

    inner = (z > 0) & (z < n - 1)

    @pl.when(inner)
    def _():
        pl.semaphore_wait(barrier, 2)

    @pl.when(jnp.logical_not(inner) & (n > 1))
    def _():
        pl.semaphore_wait(barrier, 1)

    line.begin()
    for copy in loads:
        copy.wait()

    def tiles(body):
        def step(j, carry):
            body(pl.ds(pl.multiple_of(j * tile, tile), tile))
            return carry

        lax.fori_loop(0, hid // tile, step, 0)

    def compute(g):
        span = pl.ds(pl.multiple_of(g * rows, rows), rows)

        def body(cols):
            left = x[span, :]
            mean = dot(left, m[cols, :], ((1,), (1,)))
            pert = dot(left * a[span, :], p[cols, :], ((1,), (1,)))
            part[:, cols] = scale * mean + scale * pert * s[g, :, cols].astype(jnp.float32)

        tiles(body)

    def copy(d, g):
        return remote(
            send.at[g], recv.at[d, g], s_sem.at[g], r_sem.at[d, g], dp=(z + 1 - 2 * d + n) % n
        )

    def slot(i, carry):
        t, d = i // 2, i % 2
        behind = z + d * (n - 1 - 2 * z)
        ahead = n - 1 - behind

        @pl.when((t >= behind) & (ahead > 0))
        def _():
            g = (1 - d) * (n - 1 - t + z) + d * (t - (n - 1 - z))
            compute(g)

            @pl.when(behind > 0)
            def _():
                copy(d, g).wait_recv()

                def body(cols):
                    total = part[:, cols] + recv[d, g, :, cols].astype(jnp.float32)
                    send[g, :, cols] = total.astype(send.dtype)

                tiles(body)

            @pl.when(behind == 0)
            def _():
                def body(cols):
                    send[g, :, cols] = part[:, cols].astype(send.dtype)

                tiles(body)

            copy(d, g).start()

        @pl.when(d == 1)
        def _():
            line.relay(t + 1)

        return carry

    lax.fori_loop(0, 2 * (n - 1), slot, 0)
    compute(z)

    @pl.when(z > 0)
    def _():
        copy(0, z).wait_recv()

        def body(cols):
            part[:, cols] = part[:, cols] + recv[0, z, :, cols].astype(jnp.float32)

        tiles(body)

    @pl.when(z < n - 1)
    def _():
        copy(1, z).wait_recv()

        def body(cols):
            part[:, cols] = part[:, cols] + recv[1, z, :, cols].astype(jnp.float32)

        tiles(body)

    def body(cols):
        out[:, cols] = part[:, cols]

    tiles(body)
    for g in range(n):
        @pl.when(z != g)
        def _():
            copy(0, g).wait_send()

    line.end()


def project(cid, k, half, scale, gathered, means, perturb, signs, shard):
    n = lax.axis_size("dp")
    tokens, width = gathered.shape[2:]
    hid = means.shape[1]
    rows = tokens // n
    return pl.pallas_call(
        functools.partial(project_kernel, scale, k, half),
        out_shape=[
            jax.ShapeDtypeStruct((rows, hid), jnp.float32),
            jax.ShapeDtypeStruct((n, rows, hid), jnp.bfloat16),
        ],
        in_specs=[pl.BlockSpec(memory_space=pl.ANY)] * 4 + [pl.BlockSpec(memory_space=VMEM)],
        out_specs=[pl.BlockSpec(memory_space=VMEM)] * 2,
        scratch_shapes=[
            VMEM((tokens, width), jnp.bfloat16),
            VMEM((tokens, width), jnp.bfloat16),
            VMEM((hid, width), jnp.bfloat16),
            VMEM((hid, width), jnp.bfloat16),
            VMEM((n, rows, hid), jnp.bfloat16),
            VMEM((rows, hid), jnp.float32),
            VMEM((n, rows, hid), jnp.bfloat16),
            VMEM((2, n, rows, hid), jnp.bfloat16),
            DMA((n,)),
            DMA((2, n)),
            DMA((5,)),
            DMA((2, n)),
            DMA((2, n)),
            DMA,
        ],
        compiler_params=pltpu.CompilerParams(
            collective_id=cid, has_side_effects=True, vmem_limit_bytes=60 * 2**20
        ),
        cost_estimate=pl.CostEstimate(flops=2 * 10**10, bytes_accessed=10**7, transcendentals=0),
        name=f"project{k}",
    )(gathered, means, perturb, signs, shard)


def finish_kernel(t, out, a1, rc, rx, ry, b0, b1, r0, r1, fin, s_sem, r_sem):
    (z, y, x, c), (nz, ny, nx, nc) = place()
    width = t.shape[-1]
    half = width // 2
    f32, bf16 = jnp.float32, jnp.bfloat16
    lo, hi = pl.ds(0, half), pl.ds(half, half)
    greet_axes()
    sends = []
    count = [0]

    def start(src, dst, **where):
        i = count[0]
        count[0] += 1
        copy = remote(src, dst, s_sem.at[i], r_sem.at[i], **where)
        copy.start()
        sends.append(copy)
        return copy

    def groups(body):
        def step(g, carry):
            body(g)
            return carry

        lax.fori_loop(0, nz, step, 0)

    wait = [
        start(t.at[:, :, :, (c + e) % nc], rc.at[e - 1], my=x * nc + (c + e) % nc) for e in range(1, nc)
    ]
    for copy in wait:
        copy.wait_recv()

    def add_cores(g):
        for i in range(ny):
            for j in range(nx):
                total = t[g, i, j, c].astype(f32)
                for e in range(nc - 1):
                    total = total + rc[e, g, i, j].astype(f32)
                a1[g, i, j] = total.astype(bf16)

    groups(add_cores)
    wait = [
        start(a1.at[:, :, (x + e) % nx, :, lo], rx.at[e - 1], my=((x + e) % nx) * nc + c)
        for e in range(1, nx)
    ]
    wait += [
        start(a1.at[:, (y + e) % ny, :, :, hi], ry.at[e - 1], mx=(y + e) % ny) for e in range(1, ny)
    ]
    for copy in wait:
        copy.wait_recv()

    def mine(g, i, j, cols):
        total = t[g, i, j, c, :, cols].astype(f32)
        for e in range(nc - 1):
            total = total + rc[e, g, i, j, :, cols].astype(f32)
        return total

    def low(g, i):
        total = mine(g, i, x, lo)
        for e in range(nx - 1):
            total = total + rx[e, g, i].astype(f32)
        return total

    def high(g, j):
        total = mine(g, y, j, hi)
        for e in range(ny - 1):
            total = total + ry[e, g, j].astype(f32)
        return total

    def add_first(g):
        for i in range(ny):
            b0[i, g] = low(g, i).astype(bf16)
        for j in range(nx):
            b1[j, g] = high(g, j).astype(bf16)

    groups(add_first)
    wait = [start(b0.at[(y + e) % ny], r0.at[e - 1], mx=(y + e) % ny) for e in range(1, ny)]
    wait += [
        start(b1.at[(x + e) % nx], r1.at[e - 1], my=((x + e) % nx) * nc + c) for e in range(1, nx)
    ]
    for copy in wait:
        copy.wait_recv()

    def add_second(g):
        total = low(g, y)
        for e in range(ny - 1):
            total = total + r0[e, g].astype(f32)
        fin[g, :, lo] = total.astype(bf16)
        total = high(g, x)
        for e in range(nx - 1):
            total = total + r1[e, g].astype(f32)
        fin[g, :, hi] = total.astype(bf16)

    groups(add_second)
    cols = pl.ds(pl.multiple_of(z * width, width), width)
    wait = [start(fin.at[(z + d) % nz], out.at[:, cols], dp=(z + d) % nz) for d in range(1, nz)]
    out[:, cols] = fin[z]
    for copy in wait:
        copy.wait_recv()
    for copy in sends:
        copy.wait_send()


def finish(cid, total):
    nz, ny, nx = lax.axis_size("dp"), lax.axis_size("mx"), lax.axis_size("my")
    nc = 2 if nx % 2 == 0 else 1
    nx //= nc
    tokens, width = total.shape
    rows = tokens // (nz * ny * nx * nc)
    half = width // 2
    copies = nz + ny * 2 + nx * 2 + nc
    bf16 = jnp.bfloat16
    return pl.pallas_call(
        finish_kernel,
        out_shape=jax.ShapeDtypeStruct((rows, nz * width), bf16),
        in_specs=[pl.BlockSpec(memory_space=VMEM)],
        out_specs=pl.BlockSpec(memory_space=VMEM),
        scratch_shapes=[
            VMEM((nz, ny, nx, rows, width), bf16),
            VMEM((max(nc - 1, 1), nz, ny, nx, rows, width), bf16),
            VMEM((max(nx - 1, 1), nz, ny, rows, half), bf16),
            VMEM((max(ny - 1, 1), nz, nx, rows, half), bf16),
            VMEM((ny, nz, rows, half), bf16),
            VMEM((nx, nz, rows, half), bf16),
            VMEM((max(ny - 1, 1), nz, rows, half), bf16),
            VMEM((max(nx - 1, 1), nz, rows, half), bf16),
            VMEM((nz, rows, width), bf16),
            DMA((copies,)),
            DMA((copies,)),
        ],
        compiler_params=pltpu.CompilerParams(
            collective_id=cid, has_side_effects=True, vmem_limit_bytes=32 * 2**20
        ),
        cost_estimate=pl.CostEstimate(flops=10**10, bytes_accessed=10**7, transcendentals=0),
        name=f"finish{cid}",
    )(total.reshape(nz, ny, nx, nc, rows, width))


def grad_kernel(groups, scale, hid, sign, x, a, noise, *rest):
    mean, sigma = rest[-2:]
    rows = x.shape[0] // groups
    total_mean = total_pert = None
    for g in range(groups):
        part = slice(g * rows, (g + 1) * rows)
        left = hid[part, :]
        right = x[part, :]
        m = (scale * dot(left, right, ((0,), (0,)))).astype(jnp.bfloat16)
        p = (scale * dot(left * sign[part, :], right * a[part, :], ((0,), (0,)))).astype(jnp.bfloat16)
        m, p = m.astype(jnp.float32), p.astype(jnp.float32)
        total_mean = m if g == 0 else total_mean + m
        total_pert = p if g == 0 else total_pert + p
    mean[...] = total_mean.astype(jnp.bfloat16)
    sigma[...] = (total_pert * noise[...].astype(jnp.float32)).astype(jnp.bfloat16)


def weight_grads(groups, k, half, scale, hid, sign, gathered, noise, into, begin=0):
    tokens, ff = hid.shape
    width = gathered.shape[3]
    tile = 256 if ff % 256 == 0 and begin % 256 == 0 else ff
    skip = begin // tile
    whole = lambda j: pl.BlockSpec((None, None, tokens, width), lambda i: (half, j, 0, 0))
    block = pl.BlockSpec((None, tile, width), lambda i: (k, skip + i, 0))
    cols = pl.BlockSpec((tokens, tile), lambda i: (0, i))
    signs = pl.BlockSpec((tokens, tile), lambda i: (0, skip + i))
    keep = [pl.BlockSpec(memory_space=pl.ANY)] * len(into)
    return pl.pallas_call(
        functools.partial(grad_kernel, groups, scale),
        grid=(ff // tile,),
        out_shape=[jax.ShapeDtypeStruct(noise.shape, jnp.bfloat16)] * 2,
        in_specs=[cols, signs, whole(0), whole(1), block] + keep,
        out_specs=[block, block],
        input_output_aliases={5 + i: i for i in range(len(into))},
        cost_estimate=pl.CostEstimate(
            flops=4 * tokens * ff * width, bytes_accessed=6 * ff * width, transcendentals=0
        ),
        name=f"grads{k}_{skip}",
    )(hid, sign, gathered, gathered, noise, *into)


def on_device(
    inputs,
    weight_means,
    weight_sigmas,
    weight_noise,
    input_signs,
    output_signs,
    hidden_signs,
    result_signs,
    cotangent,
):
    f32, bf16 = jnp.float32, jnp.bfloat16
    scale_in = D ** (-0.5)
    scale_out = FF ** (-0.5)
    groups = lax.axis_size("dp")

    def share(value):
        return lax.all_gather(value, "dp", axis=0, tiled=True)

    rows, full = inputs.shape
    width = full // groups
    pairs = jnp.stack([inputs, to_sign(input_signs), cotangent, to_sign(result_signs)])
    pairs = pairs.reshape(2, 2, rows, groups, width).swapaxes(2, 3)
    own_s0, own_s1 = to_sign(output_signs[0]).T, to_sign(output_signs[1]).T
    own_s2 = to_sign(hidden_signs).T
    gathered, perturb, s0 = spread(pairs, weight_sigmas, weight_noise, own_s0)
    gathered = gathered.reshape(2, 2, -1, width)
    perturb = perturb.reshape(weight_sigmas.shape)
    a, r = gathered[0, 1], gathered[1, 1]

    gate, s1 = project(2, 0, 0, scale_in, gathered, weight_means, perturb, s0, own_s1)
    up, s2 = project(3, 1, 0, scale_in, gathered, weight_means, perturb, s1, own_s2)
    gate_sig = jax.nn.sigmoid(gate)
    hidden = (gate * gate_sig * up).astype(bf16)
    hid_grad, hidden = project(4, 2, 1, scale_out, gathered, weight_means, perturb, s2, hidden)
    up_grad = share((hid_grad * gate * gate_sig).astype(bf16))
    gate_grad = (hid_grad * up * gate_sig * (1.0 + gate * (1.0 - gate_sig))).astype(bf16)
    ff = gate_grad.shape[1]
    cut = -(-ff // 512) * 256 if ff % 256 == 0 else ff
    spans = [slice(0, cut), slice(cut, ff)] if cut < ff else [slice(0, ff)]
    gate_grads = [share(gate_grad[:, span]) for span in spans]
    hidden, s0, s1, s2 = (v.reshape(-1, v.shape[2]) for v in (hidden, s0, s1, s2))

    def back(k, value, sign, span=slice(None)):
        return (
            dot(value, weight_means[k, span], ((1,), (0,))),
            dot(value * sign[:, span], perturb[k, span], ((1,), (0,))),
        )

    mean, pert = back(2, hidden, s2)
    result = finish(5, (scale_out * mean + scale_out * pert * r.astype(f32)).astype(bf16))
    grads = weight_grads(groups, 2, 1, scale_out, hidden, s2, gathered, weight_noise, ())
    up_grad, result, *grads = lax.optimization_barrier((up_grad, result, *grads))
    up_mean, up_pert = back(1, up_grad, s1)
    grads = weight_grads(groups, 1, 0, scale_in, up_grad, s1, gathered, weight_noise, grads)
    mean, pert = up_mean, up_pert
    for span, value in zip(spans, gate_grads):
        value, mean, pert, *grads = lax.optimization_barrier((value, mean, pert, *grads))
        gate_mean, gate_pert = back(0, value, s0, span)
        mean, pert = mean + gate_mean, pert + gate_pert
        if span.stop == ff:
            input_grad = finish(
                6, (scale_in * mean + scale_in * pert * a.astype(f32)).astype(bf16)
            )
        grads = weight_grads(
            groups, 0, 0, scale_in, value, s0, gathered, weight_noise, grads, span.start
        )
    mean_grad, sigma_grad = grads
    return (result, input_grad, mean_grad, sigma_grad)


def solution(mesh):
    return jax.shard_map(
        on_device,
        mesh=mesh,
        in_specs=(
            P(("dp", "mx", "my"), None),
            P(None, ("mx", "my"), "dp"),
            P(None, ("mx", "my"), "dp"),
            P(None, ("mx", "my"), "dp"),
            P(("dp", "mx", "my"), None),
            P(None, ("mx", "my"), "dp"),
            P(("mx", "my"), "dp"),
            P(("dp", "mx", "my"), None),
            P(("dp", "mx", "my"), None),
        ),
        out_specs=(
            P(("dp", "mx", "my"), None),
            P(("dp", "mx", "my"), None),
            P(None, ("mx", "my"), "dp"),
            P(None, ("mx", "my"), "dp"),
        ),
        check_vma=False,
    )
```

```python
import functools

import jax
import jax.numpy as jnp
from jax import lax
from jax.experimental import pallas as pl
from jax.experimental.pallas import tpu as pltpu
from jax.sharding import PartitionSpec as P

D = 4096
FF = 14336
MESH = pl.DeviceIdType.MESH
VMEM = pltpu.VMEM
DMA = pltpu.SemaphoreType.DMA


def to_sign(values):
    return (2 * values - 1).astype(jnp.bfloat16)


def dot(left, right, dims):
    return lax.dot_general(left, right, (dims, ((), ())), preferred_element_type=jnp.float32)


def remote(src, dst, send_sem, recv_sem, **where):
    return pltpu.make_async_remote_copy(
        src_ref=src, dst_ref=dst, send_sem=send_sem, recv_sem=recv_sem,
        device_id=where, device_id_type=MESH,
    )


def place():
    cores = 2 if lax.axis_size("my") % 2 == 0 else 1
    z, y, m = lax.axis_index("dp"), lax.axis_index("mx"), lax.axis_index("my")
    sizes = (lax.axis_size("dp"), lax.axis_size("mx"), lax.axis_size("my") // cores, cores)
    return (z, y, m // cores, m % cores), sizes


def greet_axes():
    (z, y, x, c), (nz, ny, nx, nc) = place()
    barrier = pltpu.get_barrier_semaphore()
    for d in range(1, nz):
        pl.semaphore_signal(barrier, inc=1, device_id={"dp": (z + d) % nz}, device_id_type=MESH)
    for d in range(1, ny):
        pl.semaphore_signal(barrier, inc=1, device_id={"mx": (y + d) % ny}, device_id_type=MESH)
    for d in range(1, nx):
        peer = ((x + d) % nx) * nc + c
        pl.semaphore_signal(barrier, inc=1, device_id={"my": peer}, device_id_type=MESH)
    for d in range(1, nc):
        peer = x * nc + (c + d) % nc
        pl.semaphore_signal(barrier, inc=1, device_id={"my": peer}, device_id_type=MESH)
    pl.semaphore_wait(barrier, nz + ny + nx + nc - 4)


class LineGather:
    def __init__(self, shard, full, s_sem, r_sem, own_sem):
        self.z, self.n = lax.axis_index("dp"), lax.axis_size("dp")
        self.shard, self.full, self.s_sem, self.r_sem = shard, full, s_sem, r_sem
        self.own = pltpu.make_async_copy(shard, full.at[self.z], own_sem)

    def copy(self, d, origin, src):
        return remote(
            src, self.full.at[origin], self.s_sem.at[d, origin], self.r_sem.at[d, origin],
            dp=(self.z + 1 - 2 * d + self.n) % self.n,
        )

    def begin(self):
        self.own.start()

        @pl.when(self.z < self.n - 1)
        def _():
            self.copy(0, self.z, self.shard).start()

        @pl.when(self.z > 0)
        def _():
            self.copy(1, self.z, self.shard).start()

    def relay(self, step):
        z, n = self.z, self.n
        for d in range(2):
            origin = z - step + 2 * d * step

            @pl.when((origin >= 0) & (origin < n))
            def _():
                copy = self.copy(d, origin, self.full.at[origin])
                copy.wait_recv()

                @pl.when((z < n - 1) if d == 0 else (z > 0))
                def _():
                    copy.start()

    def end(self):
        z, n = self.z, self.n
        self.own.wait()
        for origin in range(n):
            @pl.when((origin <= z) & (z < n - 1))
            def _():
                self.copy(0, origin, self.shard).wait_send()

            @pl.when((origin >= z) & (z > 0))
            def _():
                self.copy(1, origin, self.shard).wait_send()


def perturb_tiles(sigma, noise, out, wide, made, load, store):
    rows = made.shape[1]
    steps = out.shape[0] // rows

    def loads(i, slot):
        span = pl.ds(pl.multiple_of(i * rows, rows), rows)
        return (
            pltpu.make_async_copy(sigma.at[span], wide.at[slot, 0], load.at[slot, 0]),
            pltpu.make_async_copy(noise.at[span], wide.at[slot, 1], load.at[slot, 1]),
        )

    def stores(i, slot):
        span = pl.ds(pl.multiple_of(i * rows, rows), rows)
        return pltpu.make_async_copy(made.at[slot], out.at[span], store.at[slot])

    for copy in loads(0, 0):
        copy.start()

    def step(i, carry):
        slot = i % 2
        for copy in loads(i, slot):
            copy.wait()

        @pl.when(i + 1 < steps)
        def _():
            for copy in loads(i + 1, 1 - slot):
                copy.start()

        @pl.when(i >= 2)
        def _():
            stores(i - 2, slot).wait()

        product = wide[slot, 0].astype(jnp.float32) * wide[slot, 1].astype(jnp.float32)
        made[slot] = product.astype(made.dtype)
        stores(i, slot).start()
        return carry

    lax.fori_loop(0, steps, step, 0)
    for i in range(max(steps - 2, 0), steps):
        stores(i, i % 2).wait()


def spread_kernel(src, sigma, noise, shard, out, perturb, full, *scratch):
    z_s, z_r, a_s, a_r, b_s, b_r, c_s, c_r, own, g_s, g_r, g_own, wide, made, load, store = scratch
    (z, y, x, c), (nz, ny, nx, nc) = place()
    line = LineGather(shard, full, g_s, g_r, g_own)
    greet_axes()
    toward = 1 - 2 * ((2 * z) // nz)
    group = [(z + toward * k + nz) % nz for k in range(nz)]
    sends = []

    def start(copy):
        copy.start()
        sends.append(copy)
        return copy

    local = []
    for p in range(2):
        keep = pltpu.make_async_copy(src.at[p, :, z], out.at[p, :, z, y, x, c], own.at[p])
        keep.start()
        local.append(keep)
    for k in range(1, nz):
        for p in range(2):
            g = group[nz - k]
            start(remote(src.at[p, :, g], out.at[p, :, z, y, x, c], z_s.at[p, g], z_r.at[p, z], dp=g))

    def first(p, k):
        g = group[k]
        block = out.at[p, :, g, y, x, c]
        if k > 0:
            remote(src.at[p, :, g], block, z_s.at[p, g], z_r.at[p, g], dp=g).wait_recv()
        origin = src.at[p, :, g] if k == 0 else block
        if p == 0:
            return [
                start(remote(origin, block, a_s.at[p, g, e], a_r.at[p, g, e], my=((x + e) % nx) * nc + c))
                for e in range(1, nx)
            ]
        return [
            start(remote(origin, block, a_s.at[p, g, e], a_r.at[p, g, e], mx=(y + e) % ny))
            for e in range(1, ny)
        ]

    def second(p, k, before):
        g = group[k]
        for copy in before:
            copy.wait_recv()
        if k == 0:
            local[p].wait()
        if p == 0:
            block = out.at[p, :, g, y, :, c]
            return [
                start(remote(block, block, b_s.at[p, g, e], b_r.at[p, g, e], mx=(y + e) % ny))
                for e in range(1, ny)
            ]
        block = out.at[p, :, g, :, x, c]
        return [
            start(remote(block, block, b_s.at[p, g, e], b_r.at[p, g, e], my=((x + e) % nx) * nc + c))
            for e in range(1, nx)
        ]

    def third(p, k, before):
        g = group[k]
        for copy in before:
            copy.wait_recv()
        block = out.at[p, :, g, :, :, c]
        return [
            start(remote(block, block, c_s.at[p, g, e], c_r.at[p, g, e], my=x * nc + (c + e) % nc))
            for e in range(1, nc)
        ]

    a, b, last = {}, {}, []
    for p in range(2):
        a[p, 0] = first(p, 0)
    line.begin()
    perturb_tiles(sigma, noise, perturb, wide, made, load, store)
    for k in range(1, nz):
        for p in range(2):
            a[p, k] = first(p, k)
    for p in range(2):
        b[p, 0] = second(p, 0, a[p, 0])
    line.relay(1)
    for k in range(1, nz):
        for p in range(2):
            b[p, k] = second(p, k, a[p, k])
    for p in range(2):
        last += third(p, 0, b[p, 0])
    line.relay(2)
    for k in range(1, nz):
        for p in range(2):
            last += third(p, k, b[p, k])
    for step in range(3, nz):
        line.relay(step)
    for copy in last:
        copy.wait_recv()
    for copy in sends:
        copy.wait_send()
    line.end()


def spread(pairs, sigma, noise, shard):
    nz, ny, nx = lax.axis_size("dp"), lax.axis_size("mx"), lax.axis_size("my")
    nc = 2 if nx % 2 == 0 else 1
    nx //= nc
    _, _, _, rows, width = pairs.shape
    most = max(nx, ny)
    planes, hid, _ = sigma.shape
    flat = (planes * hid, width)
    fits = [t for t in range(16, 769, 16) if flat[0] % t == 0]
    tile = max(fits) if fits else hid
    anywhere = pl.BlockSpec(memory_space=pl.ANY)
    within = pl.BlockSpec(memory_space=VMEM)
    bf16 = jnp.bfloat16
    return pl.pallas_call(
        spread_kernel,
        out_shape=[
            jax.ShapeDtypeStruct((2, 2, nz, ny, nx, nc, rows, width), bf16),
            jax.ShapeDtypeStruct(flat, bf16),
            jax.ShapeDtypeStruct((nz,) + shard.shape, bf16),
        ],
        in_specs=[anywhere, anywhere, anywhere, within],
        out_specs=[anywhere, anywhere, within],
        scratch_shapes=[
            DMA((2, nz)), DMA((2, nz)),
            DMA((2, nz, most)), DMA((2, nz, most)),
            DMA((2, nz, most)), DMA((2, nz, most)),
            DMA((2, nz, nc)), DMA((2, nz, nc)),
            DMA((2,)),
            DMA((2, nz)), DMA((2, nz)), DMA,
            VMEM((2, 2, tile, width), bf16),
            VMEM((2, tile, width), bf16),
            DMA((2, 2)), DMA((2,)),
        ],
        compiler_params=pltpu.CompilerParams(
            collective_id=1, has_side_effects=True, vmem_limit_bytes=60 * 2**20
        ),
        cost_estimate=pl.CostEstimate(flops=10**10, bytes_accessed=10**7, transcendentals=0),
        name="spread",
    )(pairs, sigma.reshape(flat), noise.reshape(flat), shard)


def project_kernel(scale, k, half, gathered, means, perturb, signs, shard, out, full, *scratch):
    x, a, m, p, s, part, send, recv, s_sem, r_sem, load, g_s, g_r, g_own = scratch
    line = LineGather(shard, full, g_s, g_r, g_own)
    z, n = lax.axis_index("dp"), lax.axis_size("dp")
    rows, hid = out.shape
    sources = (gathered.at[half, 0], gathered.at[half, 1], means.at[k], perturb.at[k], signs)
    loads = [
        pltpu.make_async_copy(source, target, load.at[i])
        for i, (source, target) in enumerate(zip(sources, (x, a, m, p, s)))
    ]
    for copy in loads:
        copy.start()
    tile = 256 if hid % 256 == 0 else hid
    barrier = pltpu.get_barrier_semaphore()

    @pl.when(z > 0)
    def _():
        pl.semaphore_signal(barrier, inc=1, device_id={"dp": z - 1}, device_id_type=MESH)

    @pl.when(z < n - 1)
    def _():
        pl.semaphore_signal(barrier, inc=1, device_id={"dp": z + 1}, device_id_type=MESH)

    inner = (z > 0) & (z < n - 1)

    @pl.when(inner)
    def _():
        pl.semaphore_wait(barrier, 2)

    @pl.when(jnp.logical_not(inner) & (n > 1))
    def _():
        pl.semaphore_wait(barrier, 1)

    line.begin()
    for copy in loads:
        copy.wait()

    def tiles(body):
        def step(j, carry):
            body(pl.ds(pl.multiple_of(j * tile, tile), tile))
            return carry

        lax.fori_loop(0, hid // tile, step, 0)

    def compute(g):
        span = pl.ds(pl.multiple_of(g * rows, rows), rows)

        def body(cols):
            left = x[span, :]
            mean = dot(left, m[cols, :], ((1,), (1,)))
            pert = dot(left * a[span, :], p[cols, :], ((1,), (1,)))
            part[:, cols] = scale * mean + scale * pert * s[g, :, cols].astype(jnp.float32)

        tiles(body)

    def copy(d, g):
        return remote(
            send.at[g], recv.at[d, g], s_sem.at[g], r_sem.at[d, g], dp=(z + 1 - 2 * d + n) % n
        )

    def slot(i, carry):
        t, d = i // 2, i % 2
        behind = z + d * (n - 1 - 2 * z)
        ahead = n - 1 - behind

        @pl.when((t >= behind) & (ahead > 0))
        def _():
            g = (1 - d) * (n - 1 - t + z) + d * (t - (n - 1 - z))
            compute(g)

            @pl.when(behind > 0)
            def _():
                copy(d, g).wait_recv()

                def body(cols):
                    total = part[:, cols] + recv[d, g, :, cols].astype(jnp.float32)
                    send[g, :, cols] = total.astype(send.dtype)

                tiles(body)

            @pl.when(behind == 0)
            def _():
                def body(cols):
                    send[g, :, cols] = part[:, cols].astype(send.dtype)

                tiles(body)

            copy(d, g).start()

        @pl.when(d == 1)
        def _():
            line.relay(t + 1)

        return carry

    lax.fori_loop(0, 2 * (n - 1), slot, 0)
    compute(z)

    @pl.when(z > 0)
    def _():
        copy(0, z).wait_recv()

        def body(cols):
            part[:, cols] = part[:, cols] + recv[0, z, :, cols].astype(jnp.float32)

        tiles(body)

    @pl.when(z < n - 1)
    def _():
        copy(1, z).wait_recv()

        def body(cols):
            part[:, cols] = part[:, cols] + recv[1, z, :, cols].astype(jnp.float32)

        tiles(body)

    def body(cols):
        out[:, cols] = part[:, cols]

    tiles(body)
    for g in range(n):
        @pl.when(z != g)
        def _():
            copy(0, g).wait_send()

    line.end()


def project(cid, k, half, scale, gathered, means, perturb, signs, shard):
    n = lax.axis_size("dp")
    tokens, width = gathered.shape[2:]
    hid = means.shape[1]
    rows = tokens // n
    return pl.pallas_call(
        functools.partial(project_kernel, scale, k, half),
        out_shape=[
            jax.ShapeDtypeStruct((rows, hid), jnp.float32),
            jax.ShapeDtypeStruct((n, rows, hid), jnp.bfloat16),
        ],
        in_specs=[pl.BlockSpec(memory_space=pl.ANY)] * 4 + [pl.BlockSpec(memory_space=VMEM)],
        out_specs=[pl.BlockSpec(memory_space=VMEM)] * 2,
        scratch_shapes=[
            VMEM((tokens, width), jnp.bfloat16),
            VMEM((tokens, width), jnp.bfloat16),
            VMEM((hid, width), jnp.bfloat16),
            VMEM((hid, width), jnp.bfloat16),
            VMEM((n, rows, hid), jnp.bfloat16),
            VMEM((rows, hid), jnp.float32),
            VMEM((n, rows, hid), jnp.bfloat16),
            VMEM((2, n, rows, hid), jnp.bfloat16),
            DMA((n,)),
            DMA((2, n)),
            DMA((5,)),
            DMA((2, n)),
            DMA((2, n)),
            DMA,
        ],
        compiler_params=pltpu.CompilerParams(
            collective_id=cid, has_side_effects=True, vmem_limit_bytes=60 * 2**20
        ),
        cost_estimate=pl.CostEstimate(flops=2 * 10**10, bytes_accessed=10**7, transcendentals=0),
        name=f"project{k}",
    )(gathered, means, perturb, signs, shard)


def finish_kernel(t, out, a1, rc, rx, ry, b0, b1, r0, r1, fin, s_sem, r_sem):
    (z, y, x, c), (nz, ny, nx, nc) = place()
    width = t.shape[-1]
    half = width // 2
    f32, bf16 = jnp.float32, jnp.bfloat16
    lo, hi = pl.ds(0, half), pl.ds(half, half)
    greet_axes()
    sends = []
    count = [0]

    def start(src, dst, **where):
        i = count[0]
        count[0] += 1
        copy = remote(src, dst, s_sem.at[i], r_sem.at[i], **where)
        copy.start()
        sends.append(copy)
        return copy

    def groups(body):
        def step(g, carry):
            body(g)
            return carry

        lax.fori_loop(0, nz, step, 0)

    wait = [
        start(t.at[:, :, :, (c + e) % nc], rc.at[e - 1], my=x * nc + (c + e) % nc) for e in range(1, nc)
    ]
    for copy in wait:
        copy.wait_recv()

    def add_cores(g):
        for i in range(ny):
            for j in range(nx):
                total = t[g, i, j, c].astype(f32)
                for e in range(nc - 1):
                    total = total + rc[e, g, i, j].astype(f32)
                a1[g, i, j] = total.astype(bf16)

    groups(add_cores)
    wait = [
        start(a1.at[:, :, (x + e) % nx, :, lo], rx.at[e - 1], my=((x + e) % nx) * nc + c)
        for e in range(1, nx)
    ]
    wait += [
        start(a1.at[:, (y + e) % ny, :, :, hi], ry.at[e - 1], mx=(y + e) % ny) for e in range(1, ny)
    ]
    for copy in wait:
        copy.wait_recv()

    def mine(g, i, j, cols):
        total = t[g, i, j, c, :, cols].astype(f32)
        for e in range(nc - 1):
            total = total + rc[e, g, i, j, :, cols].astype(f32)
        return total

    def low(g, i):
        total = mine(g, i, x, lo)
        for e in range(nx - 1):
            total = total + rx[e, g, i].astype(f32)
        return total

    def high(g, j):
        total = mine(g, y, j, hi)
        for e in range(ny - 1):
            total = total + ry[e, g, j].astype(f32)
        return total

    def add_first(g):
        for i in range(ny):
            b0[i, g] = low(g, i).astype(bf16)
        for j in range(nx):
            b1[j, g] = high(g, j).astype(bf16)

    groups(add_first)
    wait = [start(b0.at[(y + e) % ny], r0.at[e - 1], mx=(y + e) % ny) for e in range(1, ny)]
    wait += [
        start(b1.at[(x + e) % nx], r1.at[e - 1], my=((x + e) % nx) * nc + c) for e in range(1, nx)
    ]
    for copy in wait:
        copy.wait_recv()

    def add_second(g):
        total = low(g, y)
        for e in range(ny - 1):
            total = total + r0[e, g].astype(f32)
        fin[g, :, lo] = total.astype(bf16)
        total = high(g, x)
        for e in range(nx - 1):
            total = total + r1[e, g].astype(f32)
        fin[g, :, hi] = total.astype(bf16)

    groups(add_second)
    cols = pl.ds(pl.multiple_of(z * width, width), width)
    wait = [start(fin.at[(z + d) % nz], out.at[:, cols], dp=(z + d) % nz) for d in range(1, nz)]
    out[:, cols] = fin[z]
    for copy in wait:
        copy.wait_recv()
    for copy in sends:
        copy.wait_send()


def finish(cid, total):
    nz, ny, nx = lax.axis_size("dp"), lax.axis_size("mx"), lax.axis_size("my")
    nc = 2 if nx % 2 == 0 else 1
    nx //= nc
    tokens, width = total.shape
    rows = tokens // (nz * ny * nx * nc)
    half = width // 2
    copies = nz + ny * 2 + nx * 2 + nc
    bf16 = jnp.bfloat16
    return pl.pallas_call(
        finish_kernel,
        out_shape=jax.ShapeDtypeStruct((rows, nz * width), bf16),
        in_specs=[pl.BlockSpec(memory_space=VMEM)],
        out_specs=pl.BlockSpec(memory_space=VMEM),
        scratch_shapes=[
            VMEM((nz, ny, nx, rows, width), bf16),
            VMEM((max(nc - 1, 1), nz, ny, nx, rows, width), bf16),
            VMEM((max(nx - 1, 1), nz, ny, rows, half), bf16),
            VMEM((max(ny - 1, 1), nz, nx, rows, half), bf16),
            VMEM((ny, nz, rows, half), bf16),
            VMEM((nx, nz, rows, half), bf16),
            VMEM((max(ny - 1, 1), nz, rows, half), bf16),
            VMEM((max(nx - 1, 1), nz, rows, half), bf16),
            VMEM((nz, rows, width), bf16),
            DMA((copies,)),
            DMA((copies,)),
        ],
        compiler_params=pltpu.CompilerParams(
            collective_id=cid, has_side_effects=True, vmem_limit_bytes=32 * 2**20
        ),
        cost_estimate=pl.CostEstimate(flops=10**10, bytes_accessed=10**7, transcendentals=0),
        name=f"finish{cid}",
    )(total.reshape(nz, ny, nx, nc, rows, width))


def grad_kernel(groups, scale, hid, sign, x, a, noise, *rest):
    mean, sigma = rest[-2:]
    rows = x.shape[0] // groups
    total_mean = total_pert = None
    for g in range(groups):
        part = slice(g * rows, (g + 1) * rows)
        left = hid[part, :]
        right = x[part, :]
        m = (scale * dot(left, right, ((0,), (0,)))).astype(jnp.bfloat16)
        p = (scale * dot(left * sign[part, :], right * a[part, :], ((0,), (0,)))).astype(jnp.bfloat16)
        m, p = m.astype(jnp.float32), p.astype(jnp.float32)
        total_mean = m if g == 0 else total_mean + m
        total_pert = p if g == 0 else total_pert + p
    mean[...] = total_mean.astype(jnp.bfloat16)
    sigma[...] = (total_pert * noise[...].astype(jnp.float32)).astype(jnp.bfloat16)


def weight_grads(groups, k, half, scale, hid, sign, gathered, noise, into, span, at=0):
    tokens = hid.shape[0]
    ff = span.stop - span.start
    width = gathered.shape[3]
    tile = 256 if all(v % 256 == 0 for v in (ff, span.start, at)) else ff
    skip, lead = span.start // tile, at // tile
    whole = lambda j: pl.BlockSpec((None, None, tokens, width), lambda i: (half, j, 0, 0))
    block = pl.BlockSpec((None, tile, width), lambda i: (k, skip + i, 0))
    cols = pl.BlockSpec((tokens, tile), lambda i: (0, lead + i))
    signs = pl.BlockSpec((tokens, tile), lambda i: (0, skip + i))
    keep = [pl.BlockSpec(memory_space=pl.ANY)] * len(into)
    return pl.pallas_call(
        functools.partial(grad_kernel, groups, scale),
        grid=(ff // tile,),
        out_shape=[jax.ShapeDtypeStruct(noise.shape, jnp.bfloat16)] * 2,
        in_specs=[cols, signs, whole(0), whole(1), block] + keep,
        out_specs=[block, block],
        input_output_aliases={5 + i: i for i in range(len(into))},
        cost_estimate=pl.CostEstimate(
            flops=4 * tokens * ff * width, bytes_accessed=6 * ff * width, transcendentals=0
        ),
        name=f"grads{k}_{skip}",
    )(hid, sign, gathered, gathered, noise, *into)


def on_device(
    inputs,
    weight_means,
    weight_sigmas,
    weight_noise,
    input_signs,
    output_signs,
    hidden_signs,
    result_signs,
    cotangent,
):
    f32, bf16 = jnp.float32, jnp.bfloat16
    scale_in = D ** (-0.5)
    scale_out = FF ** (-0.5)
    groups = lax.axis_size("dp")

    def share(value):
        return lax.all_gather(value, "dp", axis=0, tiled=True)

    rows, full = inputs.shape
    width = full // groups
    pairs = jnp.stack([inputs, to_sign(input_signs), cotangent, to_sign(result_signs)])
    pairs = pairs.reshape(2, 2, rows, groups, width).swapaxes(2, 3)
    own_s0, own_s1 = to_sign(output_signs[0]).T, to_sign(output_signs[1]).T
    own_s2 = to_sign(hidden_signs).T
    gathered, perturb, s0 = spread(pairs, weight_sigmas, weight_noise, own_s0)
    gathered = gathered.reshape(2, 2, -1, width)
    perturb = perturb.reshape(weight_sigmas.shape)
    a, r = gathered[0, 1], gathered[1, 1]

    gate, s1 = project(2, 0, 0, scale_in, gathered, weight_means, perturb, s0, own_s1)
    up, s2 = project(3, 1, 0, scale_in, gathered, weight_means, perturb, s1, own_s2)
    gate_sig = jax.nn.sigmoid(gate)
    hidden = (gate * gate_sig * up).astype(bf16)
    hid_grad, hidden = project(4, 2, 1, scale_out, gathered, weight_means, perturb, s2, hidden)
    up_grad = (hid_grad * gate * gate_sig).astype(bf16)
    gate_grad = (hid_grad * up * gate_sig * (1.0 + gate * (1.0 - gate_sig))).astype(bf16)
    ff = gate_grad.shape[1]
    lead = ff // 256 * 2 // 7 * 256 if ff % 256 == 0 else 0
    early = share(jnp.concatenate([up_grad, gate_grad[:, :lead]], axis=1))
    late = share(gate_grad[:, lead:])
    hidden, s0, s1, s2 = (v.reshape(-1, v.shape[2]) for v in (hidden, s0, s1, s2))

    def back(k, value, sign, span):
        return (
            dot(value, weight_means[k, span], ((1,), (0,))),
            dot(value * sign[:, span], perturb[k, span], ((1,), (0,))),
        )

    def grads_of(k, half, scale, value, sign, into, span, at=0):
        return weight_grads(
            groups, k, half, scale, value, sign, gathered, weight_noise, into, span, at
        )

    every, head, tail = slice(0, ff), slice(0, lead), slice(lead, ff)
    mean, pert = back(2, hidden, s2, every)
    result = finish(5, (scale_out * mean + scale_out * pert * r.astype(f32)).astype(bf16))
    grads = grads_of(2, 1, scale_out, hidden, s2, (), every)
    early, result, *grads = lax.optimization_barrier((early, result, *grads))
    mean, pert = back(1, early[:, :ff], s1, every)
    grads = grads_of(1, 0, scale_in, early, s1, grads, every)
    if lead:
        gate_mean, gate_pert = back(0, early[:, ff:], s0, head)
        mean, pert = mean + gate_mean, pert + gate_pert
        grads = grads_of(0, 0, scale_in, early, s0, grads, head, ff)
    late, mean, pert, *grads = lax.optimization_barrier((late, mean, pert, *grads))
    gate_mean, gate_pert = back(0, late, s0, tail)
    mean, pert = mean + gate_mean, pert + gate_pert
    input_grad = finish(6, (scale_in * mean + scale_in * pert * a.astype(f32)).astype(bf16))
    mean_grad, sigma_grad = grads_of(0, 0, scale_in, late, s0, grads, tail)
    return (result, input_grad, mean_grad, sigma_grad)


def solution(mesh):
    return jax.shard_map(
        on_device,
        mesh=mesh,
        in_specs=(
            P(("dp", "mx", "my"), None),
            P(None, ("mx", "my"), "dp"),
            P(None, ("mx", "my"), "dp"),
            P(None, ("mx", "my"), "dp"),
            P(("dp", "mx", "my"), None),
            P(None, ("mx", "my"), "dp"),
            P(("mx", "my"), "dp"),
            P(("dp", "mx", "my"), None),
            P(("dp", "mx", "my"), None),
        ),
        out_specs=(
            P(("dp", "mx", "my"), None),
            P(("dp", "mx", "my"), None),
            P(None, ("mx", "my"), "dp"),
            P(None, ("mx", "my"), "dp"),
        ),
        check_vma=False,
    )
```

```python
import functools

import jax
import jax.numpy as jnp
from jax import lax
from jax.experimental import pallas as pl
from jax.experimental.pallas import tpu as pltpu
from jax.sharding import PartitionSpec as P

D = 4096
FF = 14336
MESH = pl.DeviceIdType.MESH
VMEM = pltpu.VMEM
DMA = pltpu.SemaphoreType.DMA


def to_sign(values):
    return (2 * values - 1).astype(jnp.bfloat16)


def dot(left, right, dims):
    return lax.dot_general(left, right, (dims, ((), ())), preferred_element_type=jnp.float32)


def remote(src, dst, send_sem, recv_sem, **where):
    return pltpu.make_async_remote_copy(
        src_ref=src, dst_ref=dst, send_sem=send_sem, recv_sem=recv_sem,
        device_id=where, device_id_type=MESH,
    )


def place():
    cores = 2 if lax.axis_size("my") % 2 == 0 else 1
    z, y, m = lax.axis_index("dp"), lax.axis_index("mx"), lax.axis_index("my")
    sizes = (lax.axis_size("dp"), lax.axis_size("mx"), lax.axis_size("my") // cores, cores)
    return (z, y, m // cores, m % cores), sizes


def greet_axes():
    (z, y, x, c), (nz, ny, nx, nc) = place()
    barrier = pltpu.get_barrier_semaphore()
    for d in range(1, nz):
        pl.semaphore_signal(barrier, inc=1, device_id={"dp": (z + d) % nz}, device_id_type=MESH)
    for d in range(1, ny):
        pl.semaphore_signal(barrier, inc=1, device_id={"mx": (y + d) % ny}, device_id_type=MESH)
    for d in range(1, nx):
        peer = ((x + d) % nx) * nc + c
        pl.semaphore_signal(barrier, inc=1, device_id={"my": peer}, device_id_type=MESH)
    for d in range(1, nc):
        peer = x * nc + (c + d) % nc
        pl.semaphore_signal(barrier, inc=1, device_id={"my": peer}, device_id_type=MESH)
    pl.semaphore_wait(barrier, nz + ny + nx + nc - 4)


class LineGather:
    def __init__(self, shard, full, s_sem, r_sem, own_sem):
        self.z, self.n = lax.axis_index("dp"), lax.axis_size("dp")
        self.shard, self.full, self.s_sem, self.r_sem = shard, full, s_sem, r_sem
        self.own = pltpu.make_async_copy(shard, full.at[self.z], own_sem)

    def copy(self, d, origin, src):
        return remote(
            src, self.full.at[origin], self.s_sem.at[d, origin], self.r_sem.at[d, origin],
            dp=(self.z + 1 - 2 * d + self.n) % self.n,
        )

    def begin(self):
        self.own.start()

        @pl.when(self.z < self.n - 1)
        def _():
            self.copy(0, self.z, self.shard).start()

        @pl.when(self.z > 0)
        def _():
            self.copy(1, self.z, self.shard).start()

    def relay(self, step):
        z, n = self.z, self.n
        for d in range(2):
            origin = z - step + 2 * d * step

            @pl.when((origin >= 0) & (origin < n))
            def _():
                copy = self.copy(d, origin, self.full.at[origin])
                copy.wait_recv()

                @pl.when((z < n - 1) if d == 0 else (z > 0))
                def _():
                    copy.start()

    def end(self):
        z, n = self.z, self.n
        self.own.wait()
        for origin in range(n):
            @pl.when((origin <= z) & (z < n - 1))
            def _():
                self.copy(0, origin, self.shard).wait_send()

            @pl.when((origin >= z) & (z > 0))
            def _():
                self.copy(1, origin, self.shard).wait_send()


def perturb_tiles(sigma, noise, out, wide, made, load, store):
    rows = made.shape[1]
    steps = out.shape[0] // rows

    def loads(i, slot):
        span = pl.ds(pl.multiple_of(i * rows, rows), rows)
        return (
            pltpu.make_async_copy(sigma.at[span], wide.at[slot, 0], load.at[slot, 0]),
            pltpu.make_async_copy(noise.at[span], wide.at[slot, 1], load.at[slot, 1]),
        )

    def stores(i, slot):
        span = pl.ds(pl.multiple_of(i * rows, rows), rows)
        return pltpu.make_async_copy(made.at[slot], out.at[span], store.at[slot])

    for copy in loads(0, 0):
        copy.start()

    def step(i, carry):
        slot = i % 2
        for copy in loads(i, slot):
            copy.wait()

        @pl.when(i + 1 < steps)
        def _():
            for copy in loads(i + 1, 1 - slot):
                copy.start()

        @pl.when(i >= 2)
        def _():
            stores(i - 2, slot).wait()

        product = wide[slot, 0].astype(jnp.float32) * wide[slot, 1].astype(jnp.float32)
        made[slot] = product.astype(made.dtype)
        stores(i, slot).start()
        return carry

    lax.fori_loop(0, steps, step, 0)
    for i in range(max(steps - 2, 0), steps):
        stores(i, i % 2).wait()


def spread_kernel(src, sigma, noise, shard, out, perturb, full, *scratch):
    z_s, z_r, a_s, a_r, b_s, b_r, c_s, c_r, own, g_s, g_r, g_own, wide, made, load, store = scratch
    (z, y, x, c), (nz, ny, nx, nc) = place()
    line = LineGather(shard, full, g_s, g_r, g_own)
    greet_axes()
    toward = 1 - 2 * ((2 * z) // nz)
    group = [(z + toward * k + nz) % nz for k in range(nz)]
    sends = []

    def start(copy):
        copy.start()
        sends.append(copy)
        return copy

    line.begin()
    local = []
    for p in range(2):
        keep = pltpu.make_async_copy(src.at[p, :, z], out.at[p, :, z, y, x, c], own.at[p])
        keep.start()
        local.append(keep)
    for k in range(1, nz):
        for p in range(2):
            g = group[nz - k]
            start(remote(src.at[p, :, g], out.at[p, :, z, y, x, c], z_s.at[p, g], z_r.at[p, z], dp=g))

    def first(p, k):
        g = group[k]
        block = out.at[p, :, g, y, x, c]
        if k > 0:
            remote(src.at[p, :, g], block, z_s.at[p, g], z_r.at[p, g], dp=g).wait_recv()
        origin = src.at[p, :, g] if k == 0 else block
        if p == 0:
            return [
                start(remote(origin, block, a_s.at[p, g, e], a_r.at[p, g, e], my=((x + e) % nx) * nc + c))
                for e in range(1, nx)
            ]
        return [
            start(remote(origin, block, a_s.at[p, g, e], a_r.at[p, g, e], mx=(y + e) % ny))
            for e in range(1, ny)
        ]

    def second(p, k, before):
        g = group[k]
        for copy in before:
            copy.wait_recv()
        if k == 0:
            local[p].wait()
        if p == 0:
            block = out.at[p, :, g, y, :, c]
            return [
                start(remote(block, block, b_s.at[p, g, e], b_r.at[p, g, e], mx=(y + e) % ny))
                for e in range(1, ny)
            ]
        block = out.at[p, :, g, :, x, c]
        return [
            start(remote(block, block, b_s.at[p, g, e], b_r.at[p, g, e], my=((x + e) % nx) * nc + c))
            for e in range(1, nx)
        ]

    def third(p, k, before):
        g = group[k]
        for copy in before:
            copy.wait_recv()
        block = out.at[p, :, g, :, :, c]
        return [
            start(remote(block, block, c_s.at[p, g, e], c_r.at[p, g, e], my=x * nc + (c + e) % nc))
            for e in range(1, nc)
        ]

    a, b, last = {}, {}, []
    for p in range(2):
        a[p, 0] = first(p, 0)
    perturb_tiles(sigma, noise, perturb, wide, made, load, store)
    line.relay(1)
    for k in range(1, nz):
        for p in range(2):
            a[p, k] = first(p, k)
    for p in range(2):
        b[p, 0] = second(p, 0, a[p, 0])
    line.relay(2)
    for k in range(1, nz):
        for p in range(2):
            b[p, k] = second(p, k, a[p, k])
    for p in range(2):
        last += third(p, 0, b[p, 0])
    for k in range(1, nz):
        for p in range(2):
            last += third(p, k, b[p, k])
    for step in range(3, nz):
        line.relay(step)
    for copy in last:
        copy.wait_recv()
    for copy in sends:
        copy.wait_send()
    line.end()


def spread(pairs, sigma, noise, shard):
    nz, ny, nx = lax.axis_size("dp"), lax.axis_size("mx"), lax.axis_size("my")
    nc = 2 if nx % 2 == 0 else 1
    nx //= nc
    _, _, _, rows, width = pairs.shape
    most = max(nx, ny)
    planes, hid, _ = sigma.shape
    flat = (planes * hid, width)
    fits = [t for t in range(16, 769, 16) if flat[0] % t == 0]
    tile = max(fits) if fits else hid
    anywhere = pl.BlockSpec(memory_space=pl.ANY)
    within = pl.BlockSpec(memory_space=VMEM)
    bf16 = jnp.bfloat16
    return pl.pallas_call(
        spread_kernel,
        out_shape=[
            jax.ShapeDtypeStruct((2, 2, nz, ny, nx, nc, rows, width), bf16),
            jax.ShapeDtypeStruct(flat, bf16),
            jax.ShapeDtypeStruct((nz,) + shard.shape, bf16),
        ],
        in_specs=[anywhere, anywhere, anywhere, within],
        out_specs=[anywhere, anywhere, within],
        scratch_shapes=[
            DMA((2, nz)), DMA((2, nz)),
            DMA((2, nz, most)), DMA((2, nz, most)),
            DMA((2, nz, most)), DMA((2, nz, most)),
            DMA((2, nz, nc)), DMA((2, nz, nc)),
            DMA((2,)),
            DMA((2, nz)), DMA((2, nz)), DMA,
            VMEM((2, 2, tile, width), bf16),
            VMEM((2, tile, width), bf16),
            DMA((2, 2)), DMA((2,)),
        ],
        compiler_params=pltpu.CompilerParams(
            collective_id=1, has_side_effects=True, vmem_limit_bytes=60 * 2**20
        ),
        cost_estimate=pl.CostEstimate(flops=10**10, bytes_accessed=10**7, transcendentals=0),
        name="spread",
    )(pairs, sigma.reshape(flat), noise.reshape(flat), shard)


def project_kernel(scale, k, half, gathered, means, perturb, signs, shard, out, full, *scratch):
    x, a, m, p, s, part, send, recv, s_sem, r_sem, load, g_s, g_r, g_own = scratch
    line = LineGather(shard, full, g_s, g_r, g_own)
    z, n = lax.axis_index("dp"), lax.axis_size("dp")
    rows, hid = out.shape
    sources = (gathered.at[half, 0], gathered.at[half, 1], means.at[k], perturb.at[k], signs)
    loads = [
        pltpu.make_async_copy(source, target, load.at[i])
        for i, (source, target) in enumerate(zip(sources, (x, a, m, p, s)))
    ]
    for copy in loads:
        copy.start()
    tile = 256 if hid % 256 == 0 else hid
    barrier = pltpu.get_barrier_semaphore()

    @pl.when(z > 0)
    def _():
        pl.semaphore_signal(barrier, inc=1, device_id={"dp": z - 1}, device_id_type=MESH)

    @pl.when(z < n - 1)
    def _():
        pl.semaphore_signal(barrier, inc=1, device_id={"dp": z + 1}, device_id_type=MESH)

    inner = (z > 0) & (z < n - 1)

    @pl.when(inner)
    def _():
        pl.semaphore_wait(barrier, 2)

    @pl.when(jnp.logical_not(inner) & (n > 1))
    def _():
        pl.semaphore_wait(barrier, 1)

    line.begin()
    for copy in loads:
        copy.wait()

    def tiles(body):
        def step(j, carry):
            body(pl.ds(pl.multiple_of(j * tile, tile), tile))
            return carry

        lax.fori_loop(0, hid // tile, step, 0)

    def compute(g):
        span = pl.ds(pl.multiple_of(g * rows, rows), rows)

        def body(cols):
            left = x[span, :]
            mean = dot(left, m[cols, :], ((1,), (1,)))
            pert = dot(left * a[span, :], p[cols, :], ((1,), (1,)))
            part[:, cols] = scale * mean + scale * pert * s[g, :, cols].astype(jnp.float32)

        tiles(body)

    def copy(d, g):
        return remote(
            send.at[g], recv.at[d, g], s_sem.at[g], r_sem.at[d, g], dp=(z + 1 - 2 * d + n) % n
        )

    def slot(i, carry):
        t, d = i // 2, i % 2
        behind = z + d * (n - 1 - 2 * z)
        ahead = n - 1 - behind

        @pl.when((t >= behind) & (ahead > 0))
        def _():
            g = (1 - d) * (n - 1 - t + z) + d * (t - (n - 1 - z))
            compute(g)

            @pl.when(behind > 0)
            def _():
                copy(d, g).wait_recv()

                def body(cols):
                    total = part[:, cols] + recv[d, g, :, cols].astype(jnp.float32)
                    send[g, :, cols] = total.astype(send.dtype)

                tiles(body)

            @pl.when(behind == 0)
            def _():
                def body(cols):
                    send[g, :, cols] = part[:, cols].astype(send.dtype)

                tiles(body)

            copy(d, g).start()

        @pl.when(d == 1)
        def _():
            line.relay(t + 1)

        return carry

    lax.fori_loop(0, 2 * (n - 1), slot, 0)
    compute(z)

    @pl.when(z > 0)
    def _():
        copy(0, z).wait_recv()

        def body(cols):
            part[:, cols] = part[:, cols] + recv[0, z, :, cols].astype(jnp.float32)

        tiles(body)

    @pl.when(z < n - 1)
    def _():
        copy(1, z).wait_recv()

        def body(cols):
            part[:, cols] = part[:, cols] + recv[1, z, :, cols].astype(jnp.float32)

        tiles(body)

    def body(cols):
        out[:, cols] = part[:, cols]

    tiles(body)
    for g in range(n):
        @pl.when(z != g)
        def _():
            copy(0, g).wait_send()

    line.end()


def project(cid, k, half, scale, gathered, means, perturb, signs, shard):
    n = lax.axis_size("dp")
    tokens, width = gathered.shape[2:]
    hid = means.shape[1]
    rows = tokens // n
    return pl.pallas_call(
        functools.partial(project_kernel, scale, k, half),
        out_shape=[
            jax.ShapeDtypeStruct((rows, hid), jnp.float32),
            jax.ShapeDtypeStruct((n, rows, hid), jnp.bfloat16),
        ],
        in_specs=[pl.BlockSpec(memory_space=pl.ANY)] * 4 + [pl.BlockSpec(memory_space=VMEM)],
        out_specs=[pl.BlockSpec(memory_space=VMEM)] * 2,
        scratch_shapes=[
            VMEM((tokens, width), jnp.bfloat16),
            VMEM((tokens, width), jnp.bfloat16),
            VMEM((hid, width), jnp.bfloat16),
            VMEM((hid, width), jnp.bfloat16),
            VMEM((n, rows, hid), jnp.bfloat16),
            VMEM((rows, hid), jnp.float32),
            VMEM((n, rows, hid), jnp.bfloat16),
            VMEM((2, n, rows, hid), jnp.bfloat16),
            DMA((n,)),
            DMA((2, n)),
            DMA((5,)),
            DMA((2, n)),
            DMA((2, n)),
            DMA,
        ],
        compiler_params=pltpu.CompilerParams(
            collective_id=cid, has_side_effects=True, vmem_limit_bytes=60 * 2**20
        ),
        cost_estimate=pl.CostEstimate(flops=2 * 10**10, bytes_accessed=10**7, transcendentals=0),
        name=f"project{k}",
    )(gathered, means, perturb, signs, shard)


def finish_kernel(t, out, a1, rc, rx, ry, b0, b1, r0, r1, fin, s_sem, r_sem):
    (z, y, x, c), (nz, ny, nx, nc) = place()
    width = t.shape[-1]
    half = width // 2
    f32, bf16 = jnp.float32, jnp.bfloat16
    lo, hi = pl.ds(0, half), pl.ds(half, half)
    greet_axes()
    sends = []
    count = [0]

    def start(src, dst, **where):
        i = count[0]
        count[0] += 1
        copy = remote(src, dst, s_sem.at[i], r_sem.at[i], **where)
        copy.start()
        sends.append(copy)
        return copy

    def groups(body):
        def step(g, carry):
            body(g)
            return carry

        lax.fori_loop(0, nz, step, 0)

    wait = [
        start(t.at[:, :, :, (c + e) % nc], rc.at[e - 1], my=x * nc + (c + e) % nc) for e in range(1, nc)
    ]
    for copy in wait:
        copy.wait_recv()

    def add_cores(g):
        for i in range(ny):
            for j in range(nx):
                total = t[g, i, j, c].astype(f32)
                for e in range(nc - 1):
                    total = total + rc[e, g, i, j].astype(f32)
                a1[g, i, j] = total.astype(bf16)

    groups(add_cores)
    wait = [
        start(a1.at[:, :, (x + e) % nx, :, lo], rx.at[e - 1], my=((x + e) % nx) * nc + c)
        for e in range(1, nx)
    ]
    wait += [
        start(a1.at[:, (y + e) % ny, :, :, hi], ry.at[e - 1], mx=(y + e) % ny) for e in range(1, ny)
    ]
    for copy in wait:
        copy.wait_recv()

    def mine(g, i, j, cols):
        total = t[g, i, j, c, :, cols].astype(f32)
        for e in range(nc - 1):
            total = total + rc[e, g, i, j, :, cols].astype(f32)
        return total

    def low(g, i):
        total = mine(g, i, x, lo)
        for e in range(nx - 1):
            total = total + rx[e, g, i].astype(f32)
        return total

    def high(g, j):
        total = mine(g, y, j, hi)
        for e in range(ny - 1):
            total = total + ry[e, g, j].astype(f32)
        return total

    def add_first(g):
        for i in range(ny):
            b0[i, g] = low(g, i).astype(bf16)
        for j in range(nx):
            b1[j, g] = high(g, j).astype(bf16)

    groups(add_first)
    wait = [start(b0.at[(y + e) % ny], r0.at[e - 1], mx=(y + e) % ny) for e in range(1, ny)]
    wait += [
        start(b1.at[(x + e) % nx], r1.at[e - 1], my=((x + e) % nx) * nc + c) for e in range(1, nx)
    ]
    for copy in wait:
        copy.wait_recv()

    def add_second(g):
        total = low(g, y)
        for e in range(ny - 1):
            total = total + r0[e, g].astype(f32)
        fin[g, :, lo] = total.astype(bf16)
        total = high(g, x)
        for e in range(nx - 1):
            total = total + r1[e, g].astype(f32)
        fin[g, :, hi] = total.astype(bf16)

    groups(add_second)
    cols = pl.ds(pl.multiple_of(z * width, width), width)
    wait = [start(fin.at[(z + d) % nz], out.at[:, cols], dp=(z + d) % nz) for d in range(1, nz)]
    out[:, cols] = fin[z]
    for copy in wait:
        copy.wait_recv()
    for copy in sends:
        copy.wait_send()


def finish(cid, total):
    nz, ny, nx = lax.axis_size("dp"), lax.axis_size("mx"), lax.axis_size("my")
    nc = 2 if nx % 2 == 0 else 1
    nx //= nc
    tokens, width = total.shape
    rows = tokens // (nz * ny * nx * nc)
    half = width // 2
    copies = nz + ny * 2 + nx * 2 + nc
    bf16 = jnp.bfloat16
    return pl.pallas_call(
        finish_kernel,
        out_shape=jax.ShapeDtypeStruct((rows, nz * width), bf16),
        in_specs=[pl.BlockSpec(memory_space=VMEM)],
        out_specs=pl.BlockSpec(memory_space=VMEM),
        scratch_shapes=[
            VMEM((nz, ny, nx, rows, width), bf16),
            VMEM((max(nc - 1, 1), nz, ny, nx, rows, width), bf16),
            VMEM((max(nx - 1, 1), nz, ny, rows, half), bf16),
            VMEM((max(ny - 1, 1), nz, nx, rows, half), bf16),
            VMEM((ny, nz, rows, half), bf16),
            VMEM((nx, nz, rows, half), bf16),
            VMEM((max(ny - 1, 1), nz, rows, half), bf16),
            VMEM((max(nx - 1, 1), nz, rows, half), bf16),
            VMEM((nz, rows, width), bf16),
            DMA((copies,)),
            DMA((copies,)),
        ],
        compiler_params=pltpu.CompilerParams(
            collective_id=cid, has_side_effects=True, vmem_limit_bytes=32 * 2**20
        ),
        cost_estimate=pl.CostEstimate(flops=10**10, bytes_accessed=10**7, transcendentals=0),
        name=f"finish{cid}",
    )(total.reshape(nz, ny, nx, nc, rows, width))


def grad_kernel(groups, scale, hid, sign, x, a, noise, *rest):
    mean, sigma = rest[-2:]
    rows = x.shape[0] // groups
    total_mean = total_pert = None
    for g in range(groups):
        part = slice(g * rows, (g + 1) * rows)
        left = hid[part, :]
        right = x[part, :]
        m = (scale * dot(left, right, ((0,), (0,)))).astype(jnp.bfloat16)
        p = (scale * dot(left * sign[part, :], right * a[part, :], ((0,), (0,)))).astype(jnp.bfloat16)
        m, p = m.astype(jnp.float32), p.astype(jnp.float32)
        total_mean = m if g == 0 else total_mean + m
        total_pert = p if g == 0 else total_pert + p
    mean[...] = total_mean.astype(jnp.bfloat16)
    sigma[...] = (total_pert * noise[...].astype(jnp.float32)).astype(jnp.bfloat16)


def weight_grads(groups, k, half, scale, hid, sign, gathered, noise, into, span, at=0):
    tokens = hid.shape[0]
    ff = span.stop - span.start
    width = gathered.shape[3]
    tile = 256 if all(v % 256 == 0 for v in (ff, span.start, at)) else ff
    skip, lead = span.start // tile, at // tile
    whole = lambda j: pl.BlockSpec((None, None, tokens, width), lambda i: (half, j, 0, 0))
    block = pl.BlockSpec((None, tile, width), lambda i: (k, skip + i, 0))
    cols = pl.BlockSpec((tokens, tile), lambda i: (0, lead + i))
    signs = pl.BlockSpec((tokens, tile), lambda i: (0, skip + i))
    keep = [pl.BlockSpec(memory_space=pl.ANY)] * len(into)
    return pl.pallas_call(
        functools.partial(grad_kernel, groups, scale),
        grid=(ff // tile,),
        out_shape=[jax.ShapeDtypeStruct(noise.shape, jnp.bfloat16)] * 2,
        in_specs=[cols, signs, whole(0), whole(1), block] + keep,
        out_specs=[block, block],
        input_output_aliases={5 + i: i for i in range(len(into))},
        cost_estimate=pl.CostEstimate(
            flops=4 * tokens * ff * width, bytes_accessed=6 * ff * width, transcendentals=0
        ),
        name=f"grads{k}_{skip}",
    )(hid, sign, gathered, gathered, noise, *into)


def on_device(
    inputs,
    weight_means,
    weight_sigmas,
    weight_noise,
    input_signs,
    output_signs,
    hidden_signs,
    result_signs,
    cotangent,
):
    f32, bf16 = jnp.float32, jnp.bfloat16
    scale_in = D ** (-0.5)
    scale_out = FF ** (-0.5)
    groups = lax.axis_size("dp")

    def share(value):
        return lax.all_gather(value, "dp", axis=0, tiled=True)

    rows, full = inputs.shape
    width = full // groups
    pairs = jnp.stack([inputs, to_sign(input_signs), cotangent, to_sign(result_signs)])
    pairs = pairs.reshape(2, 2, rows, groups, width).swapaxes(2, 3)
    own_s0, own_s1 = to_sign(output_signs[0]).T, to_sign(output_signs[1]).T
    own_s2 = to_sign(hidden_signs).T
    gathered, perturb, s0 = spread(pairs, weight_sigmas, weight_noise, own_s0)
    gathered = gathered.reshape(2, 2, -1, width)
    perturb = perturb.reshape(weight_sigmas.shape)
    a, r = gathered[0, 1], gathered[1, 1]

    gate, s1 = project(2, 0, 0, scale_in, gathered, weight_means, perturb, s0, own_s1)
    up, s2 = project(3, 1, 0, scale_in, gathered, weight_means, perturb, s1, own_s2)
    gate_sig = jax.nn.sigmoid(gate)
    hidden = (gate * gate_sig * up).astype(bf16)
    hid_grad, hidden = project(4, 2, 1, scale_out, gathered, weight_means, perturb, s2, hidden)
    up_grad = (hid_grad * gate * gate_sig).astype(bf16)
    gate_grad = (hid_grad * up * gate_sig * (1.0 + gate * (1.0 - gate_sig))).astype(bf16)
    ff = gate_grad.shape[1]
    lead = ff // 256 * 2 // 7 * 256 if ff % 256 == 0 else 0
    early = share(jnp.concatenate([up_grad, gate_grad[:, :lead]], axis=1))
    late = share(gate_grad[:, lead:])
    hidden, s0, s1, s2 = (v.reshape(-1, v.shape[2]) for v in (hidden, s0, s1, s2))

    def back(k, value, sign, span):
        return (
            dot(value, weight_means[k, span], ((1,), (0,))),
            dot(value * sign[:, span], perturb[k, span], ((1,), (0,))),
        )

    def grads_of(k, half, scale, value, sign, into, span, at=0):
        return weight_grads(
            groups, k, half, scale, value, sign, gathered, weight_noise, into, span, at
        )

    every, head, tail = slice(0, ff), slice(0, lead), slice(lead, ff)
    mean, pert = back(2, hidden, s2, every)
    result = finish(5, (scale_out * mean + scale_out * pert * r.astype(f32)).astype(bf16))
    grads = grads_of(2, 1, scale_out, hidden, s2, (), every)
    early, result, *grads = lax.optimization_barrier((early, result, *grads))
    mean, pert = back(1, early[:, :ff], s1, every)
    grads = grads_of(1, 0, scale_in, early, s1, grads, every)
    if lead:
        gate_mean, gate_pert = back(0, early[:, ff:], s0, head)
        mean, pert = mean + gate_mean, pert + gate_pert
        grads = grads_of(0, 0, scale_in, early, s0, grads, head, ff)
    late, mean, pert, *grads = lax.optimization_barrier((late, mean, pert, *grads))
    gate_mean, gate_pert = back(0, late, s0, tail)
    mean, pert = mean + gate_mean, pert + gate_pert
    input_grad = finish(6, (scale_in * mean + scale_in * pert * a.astype(f32)).astype(bf16))
    mean_grad, sigma_grad = grads_of(0, 0, scale_in, late, s0, grads, tail)
    return (result, input_grad, mean_grad, sigma_grad)


def solution(mesh):
    return jax.shard_map(
        on_device,
        mesh=mesh,
        in_specs=(
            P(("dp", "mx", "my"), None),
            P(None, ("mx", "my"), "dp"),
            P(None, ("mx", "my"), "dp"),
            P(None, ("mx", "my"), "dp"),
            P(("dp", "mx", "my"), None),
            P(None, ("mx", "my"), "dp"),
            P(("mx", "my"), "dp"),
            P(("dp", "mx", "my"), None),
            P(("dp", "mx", "my"), None),
        ),
        out_specs=(
            P(("dp", "mx", "my"), None),
            P(("dp", "mx", "my"), None),
            P(None, ("mx", "my"), "dp"),
            P(None, ("mx", "my"), "dp"),
        ),
        check_vma=False,
    )
```
